32 devices in a mesh: seq: 8 (over y, x, core), head: 4 (over z).
Axes of the slice: x: 2, y: 2, z: 4, core: 2. Of those that a mesh axis runs over, the one named last changes fastest.
Arguments:
- lat_query: bfloat16 [1024, 73728], P('seq', 'head'), may hold values from -6 to 6
- lat_keys: bfloat16 [1024, 576], P('seq'), may hold values from -6 to 6
- normalizer: float32 [1024, 128], P('seq'), may hold values from 3 to 7
- lookback: int32 [1024], P('seq'), may hold values from 1 to 1024
- index_query: bfloat16 [1024, 8192], P(('seq', 'head')), may hold values from -20 to 20
- index_keys: bfloat16 [1024, 128], P('seq'), may hold values from -6 to 6
- index_weight: float32 [1024, 64], P(('seq', 'head')), may hold values from 0.25 to 2
Outputs:
- grad_query: float32 [1024, 8192], P(('seq', 'head'))
- grad_weight: float32 [1024, 64], P(('seq', 'head'))
- grad_key: float32 [1024, 128], P(('seq', 'head'))
The draws below stay inside these ranges and needn't reach their ends.
All inputs are finite; a program needn't handle non-finite values.
Results may differ from the reference program's by a relative error of at most 0.0029.
Values may be sent and summed in bfloat16 or wider, within the bound.
No kernel may reach another device: no remote copies, remote signals or barrier semaphores. Data moves between devices by JAX's collectives and lax.ppermute only.
A program may use at most 64 MiB of HBM per device.

```python
import math
import jax
import jax.numpy as jnp
from jax import lax

HEADS = 128
KDIM = 576
IHEADS = 64
IDIM = 128
SEQ_LEN = 1024


def index_pair(key):
    base_key = jax.random.fold_in(key, 7101)
    key_values = jnp.clip(jax.random.normal(jax.random.fold_in(base_key, 1), (SEQ_LEN, IDIM), jnp.float32), -5.0, 5.0)
    query_values = jnp.clip(jax.random.normal(jax.random.fold_in(base_key, 2), (SEQ_LEN, IHEADS, IDIM), jnp.float32), -5.0, 5.0)
    return (query_values.reshape(SEQ_LEN, IHEADS * IDIM), key_values)


def draw_index_query(key, part):
    return index_pair(key)[0].astype(jnp.bfloat16)


def draw_index_keys(key, part):
    return index_pair(key)[1].astype(jnp.bfloat16)


def plant(drawn, own_key, low, high):
    extent = drawn.shape
    index_at = [jax.random.randint(jax.random.fold_in(own_key, axis), (), 0, extent[axis]) for axis in range(len(extent))]
    drawn = drawn.at[tuple(index_at)].set(low)
    longest = extent.index(max(extent))
    index_at[longest] = (index_at[longest] + 1) % extent[longest]
    return drawn.at[tuple(index_at)].set(high)


def steps_of(stream_key, extent, split, low, largest):
    def one(position, shards_of):
        steps = jax.random.uniform(jax.random.fold_in(jax.random.fold_in(stream_key, 6), position), (shards_of,), jnp.float32, low / len(split), largest / len(split))
        return jnp.repeat(jnp.exp(steps), extent[position] // shards_of).reshape((-1,) + (1,) * (len(extent) - position - 1))

    gain = one(*split[0])
    for cut in split[1:]:
        gain = gain * one(*cut)
    return gain


def gaussian(stream_key, dims, deviation, most, cuts=(), kind=jnp.bfloat16):
    result = deviation * jax.random.normal(stream_key, dims, jnp.float32)
    if cuts:
        result = result * steps_of(stream_key, dims, cuts, -0.22, 0.18)
    return jnp.clip(result, -most, most).astype(kind)


def setup_inputs(seed: int = 0) -> dict:
    seeds = jax.random.split(jax.random.key(seed), 8)
    return {
        "lat_query": gaussian(seeds[0], (SEQ_LEN, HEADS * KDIM), 1.0, 6.0, ((0, 8), (1, 4))),
        "lat_keys": gaussian(seeds[1], (SEQ_LEN, KDIM), 1.0, 6.0, ((0, 8),)),
        "normalizer": jnp.clip(3.0 + 4.0 * jax.random.uniform(seeds[2], (SEQ_LEN, HEADS), jnp.float32) ** steps_of(seeds[2], (SEQ_LEN, HEADS), ((0, 8),), -0.2, 0.2), 3.0, 7.0),
        "lookback": plant(jax.random.randint(seeds[3], (SEQ_LEN,), 1, SEQ_LEN + 1), jax.random.fold_in(seeds[3], 1), 1, SEQ_LEN).astype(jnp.int32),
        "index_query": draw_index_query(jax.random.fold_in(seeds[7], 71), 0),
        "index_keys": draw_index_keys(jax.random.fold_in(seeds[7], 71), 0),
        "index_weight": jnp.clip(jnp.exp(math.log(2.0) - 2.0794415 * jax.random.uniform(seeds[6], (SEQ_LEN, IHEADS), jnp.float32) ** steps_of(seeds[6], (SEQ_LEN, IHEADS), ((0, 32),), -0.2, 0.2)), 0.25, 2.0),
    }


def index_pass(query, weight, target, key_rows, row_pos, row_low):
    row_count = query.shape[0]
    head_count = weight.shape[1]
    key_depth = key_rows.shape[1]
    seq_total = key_rows.shape[0]
    block_rows = min(512, seq_total)
    blocks = seq_total // block_rows
    flat_query = query.reshape(row_count * head_count, key_depth)
    flat_weight = weight.reshape(row_count * head_count)
    factor = key_depth ** -0.5

    def scores(block_index):
        key_part = lax.dynamic_slice_in_dim(key_rows, block_index * block_rows, block_rows, 0)
        inner = lax.dot_general(flat_query, key_part, (((1,), (1,)), ((), ())), preferred_element_type=jnp.float32) * factor
        active = jnp.maximum(inner, 0.0)
        summed = jnp.sum((active * flat_weight[:, None]).reshape(row_count, head_count, block_rows), axis=1)
        key_pos = block_index * block_rows + jnp.arange(block_rows, dtype=jnp.int32)
        visible = (key_pos[None, :] <= row_pos[:, None]) & (key_pos[None, :] >= row_low[:, None])
        return key_part, inner, active, summed, visible

    def first_pass(running, block_index):
        row_top, row_mass = running
        _, _, _, summed, visible = scores(block_index)
        summed = jnp.where(visible, summed, -jnp.inf)
        new_top = jnp.maximum(row_top, jnp.max(summed, axis=1))
        row_mass = row_mass * jnp.exp(row_top - new_top) + jnp.sum(jnp.exp(summed - new_top[:, None]), axis=1)
        return (new_top, row_mass), None

    start_state = (jnp.full((row_count,), -1e30, jnp.float32), jnp.zeros((row_count,), jnp.float32))
    (row_top, row_mass), _ = lax.scan(first_pass, start_state, jnp.arange(blocks, dtype=jnp.int32))

    def second_pass(running, block_index):
        d_query, d_weight = running
        key_part, inner, active, summed, visible = scores(block_index)
        predicted = jnp.where(visible, jnp.exp(summed - row_top[:, None]) / row_mass[:, None], 0.0)
        target_block = lax.dynamic_slice_in_dim(target, block_index * block_rows, block_rows, 1)
        gap_term = predicted - target_block
        d_weight = d_weight + jnp.sum(active.reshape(row_count, head_count, block_rows) * gap_term[:, None, :], axis=2)
        spread = (gap_term[:, None, :] * weight[:, :, None]).reshape(row_count * head_count, block_rows) * factor
        slopes = jnp.where(inner > 0, spread, 0.0).astype(jnp.bfloat16)
        d_query = d_query + jnp.dot(slopes, key_part, preferred_element_type=jnp.float32)
        d_key = lax.dot_general(slopes, flat_query, (((0,), (0,)), ((), ())), preferred_element_type=jnp.float32)
        return (d_query, d_weight), d_key

    start_grads = (jnp.zeros((row_count * head_count, key_depth), jnp.float32), jnp.zeros((row_count, head_count), jnp.float32))
    (d_query, d_weight), d_key = lax.scan(second_pass, start_grads, jnp.arange(blocks, dtype=jnp.int32))
    return d_query.reshape(row_count, head_count * key_depth), d_weight, d_key.reshape(seq_total, key_depth)


def attention_mass(lat_query, lat_keys, normalizer, lookback):
    seq_total = lat_query.shape[0]
    block_rows = min(512, seq_total)
    score_scale = KDIM ** -0.5
    key_full = lat_keys.astype(jnp.float32)
    pieces = []
    for block_index in range(seq_total // block_rows):
        begin = block_index * block_rows
        finish = begin + block_rows
        query_block = lat_query[begin:finish].reshape(block_rows, HEADS, KDIM).astype(jnp.float32)
        query_block = jnp.transpose(query_block, (1, 0, 2))
        offsets = jnp.transpose(normalizer[begin:finish])
        key_block = key_full[:finish]

        def head_step(summed, inputs):
            query_head, offset_head = inputs
            scores = jnp.dot(query_head, key_block.T, preferred_element_type=jnp.float32, precision=lax.Precision.HIGHEST)
            return summed + jnp.exp(scores * score_scale - offset_head[:, None]), None

        summed, _ = lax.scan(head_step, jnp.zeros((block_rows, finish), jnp.float32), (query_block, offsets))
        query_pos = begin + jnp.arange(block_rows, dtype=jnp.int32)
        query_low = query_pos - lookback[begin:finish]
        key_pos = jnp.arange(finish, dtype=jnp.int32)
        visible = (key_pos[None, :] <= query_pos[:, None]) & (key_pos[None, :] >= query_low[:, None])
        summed = jnp.where(visible, summed, 0.0)
        pieces.append(jnp.concatenate([summed, jnp.zeros((block_rows, seq_total - finish), jnp.float32)], axis=1))
    return jnp.concatenate(pieces, axis=0)


def reference(lat_query, lat_keys, normalizer, lookback, index_query, index_keys, index_weight):
    seq_total = lat_query.shape[0]
    mass = attention_mass(lat_query, lat_keys, normalizer, lookback)
    target = mass / jnp.sum(mass, axis=1, keepdims=True)
    group_rows = min(64, seq_total)
    positions = jnp.arange(seq_total, dtype=jnp.int32)
    lows = positions - lookback

    def group_step(key_sum, group_index):
        begin = (group_index * group_rows).astype(jnp.int32)
        query_rows = lax.dynamic_slice_in_dim(index_query, begin, group_rows, 0)
        weight_rows = lax.dynamic_slice_in_dim(index_weight, begin, group_rows, 0)
        target_rows = lax.dynamic_slice_in_dim(target, begin, group_rows, 0)
        pos_rows = lax.dynamic_slice_in_dim(positions, begin, group_rows, 0)
        low_rows = lax.dynamic_slice_in_dim(lows, begin, group_rows, 0)
        d_query, d_weight, d_key = index_pass(query_rows, weight_rows, target_rows, index_keys, pos_rows, low_rows)
        return key_sum + d_key, (d_query, d_weight)

    key_sum, (d_query, d_weight) = lax.scan(group_step, jnp.zeros((seq_total, IDIM), jnp.float32), jnp.arange(seq_total // group_rows, dtype=jnp.int32))
    return d_query.reshape(seq_total, IHEADS * IDIM), d_weight.reshape(seq_total, IHEADS), key_sum
```

```python
import functools
import math

import jax
import jax.numpy as jnp
from jax import lax
from jax.experimental import pallas as pl
from jax.experimental.pallas import tpu as pltpu
from jax.sharding import PartitionSpec as P

KDIM = 576
LANES = 128
LOG2E = 1.0 / math.log(2.0)


def shape_of(dims, kind):
    return jax.ShapeDtypeStruct(dims, kind)


def full_spec(dims):
    return pl.BlockSpec(dims, lambda *_: (0,) * len(dims))


def spread_kernel(first, rows, norm_ref, weight_ref, look_ref, off_ref, scale_ref, low_ref, tall):
    heads, local_rows, _ = off_ref.shape
    turn = lax.axis_index("head") * heads
    offsets = norm_ref[...] * LOG2E
    width = offsets.shape[1]
    offsets = pltpu.roll(offsets, lax.rem(width - turn, width), 1)
    for head in range(heads):
        off_ref[head] = jnp.broadcast_to(offsets[:, head : head + 1], (local_rows, LANES))
    weights = weight_ref[...] * first
    for head in range(scale_ref.shape[0]):
        scale_ref[head] = jnp.broadcast_to(weights[:, head : head + 1], (rows, LANES))
    look = jnp.broadcast_to(look_ref[...].astype(jnp.float32), (LANES, look_ref.shape[1]))
    tall[...] = jnp.transpose(look)
    low_ref[...] = tall[pl.ds(lax.axis_index("head") * rows, rows), :]


def spread(normalizer, weight, lookback, heads, factor):
    rows, index_heads = weight.shape
    local_rows = normalizer.shape[0]
    out = (
        shape_of((heads, local_rows, LANES), jnp.float32),
        shape_of((index_heads, rows, LANES), jnp.float32),
        shape_of((rows, LANES), jnp.float32),
    )
    return pl.pallas_call(
        functools.partial(spread_kernel, factor, rows),
        out_shape=out,
        scratch_shapes=[pltpu.VMEM((local_rows, LANES), jnp.float32)],
        compiler_params=pltpu.CompilerParams(vmem_limit_bytes=16 << 20),
        cost_estimate=pl.CostEstimate(flops=4_000_000, bytes_accessed=0, transcendentals=0),
        name="spread",
    )(normalizer, weight, lookback.reshape(1, local_rows))


def mass_kernel(slots, group, query_ref, off_ref, *refs):
    blocks = refs[:slots]
    outs = refs[slots:-2]
    keys, acc = refs[-2:]
    step = pl.program_id(0)
    steps = pl.num_programs(0)
    pad = LANES - KDIM % LANES
    depth = KDIM + pad
    tiles, local_rows, wide = acc.shape
    per_tile = wide // LANES

    @pl.when(step == 0)
    def _():
        acc[...] = jnp.zeros_like(acc)
        for tile in range(tiles):
            keys[tile, :pad] = jnp.zeros((pad, wide), keys.dtype)
            keys[tile, pad + KDIM :] = jnp.zeros((pad, wide), keys.dtype)
            for part in range(per_tile):
                keys[tile, pad : pad + KDIM, part * LANES : (part + 1) * LANES] = blocks[
                    tile * per_tile + part
                ][:KDIM]

    scale = KDIM ** (-0.5) * LOG2E

    @pl.loop(0, tiles)
    def _(tile):
        total = acc[tile]
        for odd in range(2):
            begin = 0 if odd else pad
            picked = [
                query_ref[:, head * KDIM - (pad if odd else 0) : head * KDIM - (pad if odd else 0) + depth]
                for head in range(odd, group, 2)
            ]
            scores = jnp.dot(
                jnp.concatenate(picked, axis=0),
                keys[tile, begin : begin + depth],
                preferred_element_type=jnp.float32,
            )
            for place, head in enumerate(range(odd, group, 2)):
                offset = off_ref[head]
                part = scores[place * local_rows : (place + 1) * local_rows]
                total = total + jnp.exp2(part * scale - jnp.concatenate([offset] * per_tile, axis=1))
        acc[tile] = total

    @pl.when(step == steps - 1)
    def _():
        own, sends = outs[0], outs[1:]
        rows = own.shape[0]
        size = len(sends) + 1
        me = lax.axis_index("head")
        for tile in range(tiles):
            lanes = slice(tile * wide, (tile + 1) * wide)
            own[:, lanes] = acc[tile, pl.ds(me * rows, rows), :]
            for hop, send in enumerate(sends):
                there = lax.rem(me + hop + 1, size)
                send[:, lanes] = acc[tile, pl.ds(there * rows, rows), :].astype(send.dtype)


def attention_mass(lat_query, offsets, blocks, rows, peers):
    local_rows = lat_query.shape[0]
    heads = offsets.shape[0]
    group = min(8, heads)
    slots = len(blocks)
    wide = 2 * LANES
    tiles = slots * LANES // wide
    pad = LANES - KDIM % LANES
    part = shape_of((rows, slots * LANES), jnp.bfloat16)
    outs = (shape_of(part.shape, jnp.float32),) + (part,) * (peers - 1)
    return pl.pallas_call(
        functools.partial(mass_kernel, slots, group),
        out_shape=outs,
        grid=(heads // group,),
        in_specs=[
            pl.BlockSpec((local_rows, group * KDIM), lambda step: (0, step)),
            pl.BlockSpec((group, local_rows, LANES), lambda step: (step, 0, 0)),
        ]
        + [full_spec(block.shape) for block in blocks],
        out_specs=[full_spec(out.shape) for out in outs],
        scratch_shapes=[
            pltpu.VMEM((tiles, KDIM + 2 * pad, wide), jnp.bfloat16),
            pltpu.VMEM((tiles, local_rows, wide), jnp.float32),
        ],
        compiler_params=pltpu.CompilerParams(vmem_limit_bytes=20 << 20),
        cost_estimate=pl.CostEstimate(
            flops=2 * local_rows * heads * KDIM * slots * LANES, bytes_accessed=0, transcendentals=0
        ),
        name="mass",
    )(lat_query, offsets, *blocks)


def stack_heads(value, heads, dims):
    parts = [value[:, head * dims : (head + 1) * dims] for head in range(heads)]
    if value.shape[0] % 16 == 0:
        return jnp.concatenate(parts, axis=0)
    parts = [part.astype(jnp.float32) for part in parts]
    return jnp.concatenate(parts, axis=0).astype(value.dtype)


def score_kernel(slots, query_ref, scale_ref, low_ref, *refs):
    blocks = refs[:slots]
    active_ref, predicted_ref, keys, score = refs[slots:]
    step = pl.program_id(0)
    heads, rows, seq_total = active_ref.shape
    dims = keys.shape[1]

    @pl.when(step == 0)
    def _():
        score[...] = jnp.zeros_like(score)
        for slot in range(slots):
            keys[slot * LANES : (slot + 1) * LANES] = blocks[slot][KDIM:]

    stacked = stack_heads(query_ref[...], heads, dims)
    wide = 2 * LANES
    for begin in range(0, seq_total, wide):
        inner = lax.dot_general(
            stacked,
            keys[begin : begin + wide],
            (((1,), (1,)), ((), ())),
            preferred_element_type=jnp.float32,
        )
        total = score[:, begin : begin + wide]
        for head in range(heads):
            active = jnp.maximum(inner[head * rows : (head + 1) * rows], 0.0)
            active_ref[head, :, begin : begin + wide] = active
            total = total + active * jnp.concatenate([scale_ref[head]] * 2, axis=1)
        score[:, begin : begin + wide] = total

    @pl.when(step == pl.num_programs(0) - 1)
    def _():
        seq = lax.axis_index("seq")
        query_pos = (
            (seq * lax.axis_size("head") + lax.axis_index("head")) * rows
            + lax.broadcasted_iota(jnp.int32, (rows, LANES), 0)
        )
        low = query_pos - low_ref[...].astype(jnp.int32)
        lane = lax.broadcasted_iota(jnp.int32, (rows, LANES), 1)
        seen = []
        for slot in range(slots):
            key_pos = jnp.bitwise_xor(seq, slot) * LANES + lane
            seen.append((key_pos <= query_pos) & (key_pos >= low))
        parts = [score[:, slot * LANES : (slot + 1) * LANES] for slot in range(slots)]
        parts = [jnp.where(see, part, -jnp.inf) for see, part in zip(seen, parts)]
        top = functools.reduce(jnp.maximum, parts)
        top = jnp.max(top, axis=1, keepdims=True)
        parts = [jnp.exp(part - top) for part in parts]
        mass = jnp.sum(functools.reduce(jnp.add, parts), axis=1, keepdims=True)
        for slot in range(slots):
            predicted_ref[:, slot * LANES : (slot + 1) * LANES] = jnp.where(
                seen[slot], parts[slot] / mass, -1.0
            )


def index_scores(index_query, scales, lows, blocks, dims):
    rows = index_query.shape[0]
    index_heads = scales.shape[0]
    group = min(8, index_heads)
    slots = len(blocks)
    seq_total = slots * LANES
    return pl.pallas_call(
        functools.partial(score_kernel, slots),
        out_shape=(
            shape_of((index_heads, rows, seq_total), jnp.float32),
            shape_of((rows, seq_total), jnp.float32),
            shape_of((seq_total, dims), jnp.bfloat16),
        ),
        grid=(index_heads // group,),
        in_specs=[
            pl.BlockSpec((rows, group * dims), lambda step: (0, step)),
            pl.BlockSpec((group, rows, LANES), lambda step: (step, 0, 0)),
            full_spec(lows.shape),
        ]
        + [full_spec(block.shape) for block in blocks],
        out_specs=[
            pl.BlockSpec((group, rows, seq_total), lambda step: (step, 0, 0)),
            full_spec((rows, seq_total)),
            full_spec((seq_total, dims)),
        ],
        scratch_shapes=[pltpu.VMEM((rows, seq_total), jnp.float32)],
        compiler_params=pltpu.CompilerParams(vmem_limit_bytes=20 << 20),
        cost_estimate=pl.CostEstimate(
            flops=8 * rows * index_heads * seq_total * dims, bytes_accessed=0, transcendentals=0
        ),
        name="scores",
    )(index_query, scales, lows, *blocks)


def grads_kernel(peers, factor, own_ref, *refs):
    others = refs[: peers - 1]
    predicted_ref, active_ref, scale_ref, query_ref, keys_ref = refs[peers - 1 : peers + 4]
    grad_query_ref, grad_weight_ref, grad_key_ref, gap_ref, tall, weight_sum = refs[peers + 4 :]
    step = pl.program_id(0)
    heads, rows, seq_total = active_ref.shape
    dims = keys_ref.shape[1]
    slots = seq_total // LANES

    @pl.when(step == 0)
    def _():
        tall[...] = jnp.zeros_like(tall)
        weight_sum[...] = jnp.zeros_like(weight_sum)
        predicted = predicted_ref[...]
        seen = predicted >= 0.0
        mass = own_ref[...]
        for other in others:
            mass = mass + other[...].astype(jnp.float32)
        mass = jnp.where(seen, mass, 0.0)
        target = mass / jnp.sum(mass, axis=1, keepdims=True)
        gap_ref[...] = jnp.where(seen, predicted - target, 0.0)

    gap = gap_ref[...]
    lane = lax.broadcasted_iota(jnp.int32, (rows, LANES), 1)
    sums = weight_sum[...]
    slopes = []
    for head in range(heads):
        active = active_ref[head]
        product = active * gap
        partial = functools.reduce(
            jnp.add, [product[:, slot * LANES : (slot + 1) * LANES] for slot in range(slots)]
        )
        partial = jnp.sum(partial, axis=1, keepdims=True)
        sums = jnp.where(lane == step * heads + head, partial, sums)
        spread_gap = gap * jnp.concatenate([scale_ref[head]] * slots, axis=1)
        slope = jnp.where(active > 0.0, spread_gap, 0.0)
        slopes.append(slope if rows % 16 else slope.astype(jnp.bfloat16))
    weight_sum[...] = sums
    slopes = jnp.concatenate(slopes, axis=0).astype(jnp.bfloat16)
    grad_query = jnp.dot(slopes, keys_ref[...], preferred_element_type=jnp.float32)
    for head in range(heads):
        grad_query_ref[:, head * dims : (head + 1) * dims] = grad_query[head * rows : (head + 1) * rows]
    stacked = stack_heads(query_ref[...], heads, dims)
    tall[...] += lax.dot_general(
        stacked, slopes, (((0,), (0,)), ((), ())), preferred_element_type=jnp.float32
    )

    @pl.when(step == pl.num_programs(0) - 1)
    def _():
        grad_weight_ref[...] = sums[:, : grad_weight_ref.shape[1]] * factor
        seq = lax.axis_index("seq")
        for slot in range(slots):
            begin = pl.multiple_of(jnp.bitwise_xor(seq, slot) * LANES, LANES)
            part = jnp.transpose(tall[:, slot * LANES : (slot + 1) * LANES])
            grad_key_ref[pl.ds(begin, LANES), :] = part.astype(grad_key_ref.dtype)


def index_grads(own, others, predicted, active, scales, index_query, keys, factor):
    index_heads, rows, seq_total = active.shape
    dims = keys.shape[1]
    group = min(8, index_heads)
    peers = len(others) + 1
    flat = full_spec((rows, seq_total))
    return pl.pallas_call(
        functools.partial(grads_kernel, peers, factor),
        out_shape=(
            shape_of((rows, index_heads * dims), jnp.float32),
            shape_of((rows, index_heads), jnp.float32),
            shape_of((seq_total, dims), jnp.bfloat16),
        ),
        grid=(index_heads // group,),
        in_specs=[flat] * (peers + 1)
        + [
            pl.BlockSpec((group, rows, seq_total), lambda step: (step, 0, 0)),
            pl.BlockSpec((group, rows, LANES), lambda step: (step, 0, 0)),
            pl.BlockSpec((rows, group * dims), lambda step: (0, step)),
            full_spec(keys.shape),
        ],
        out_specs=[
            pl.BlockSpec((rows, group * dims), lambda step: (0, step)),
            full_spec((rows, index_heads)),
            full_spec((seq_total, dims)),
        ],
        scratch_shapes=[
            pltpu.VMEM((rows, seq_total), jnp.float32),
            pltpu.VMEM((dims, seq_total), jnp.float32),
            pltpu.VMEM((rows, LANES), jnp.float32),
        ],
        compiler_params=pltpu.CompilerParams(vmem_limit_bytes=20 << 20),
        cost_estimate=pl.CostEstimate(
            flops=8 * rows * index_heads * seq_total * dims, bytes_accessed=0, transcendentals=0
        ),
        name="grads",
    )(own, *others, predicted, active, scales, index_query, keys)


def per_device(lat_query, lat_keys, normalizer, lookback, index_query, index_keys, index_weight):
    seq_count = lax.axis_size("seq")
    peers = lax.axis_size("head")
    heads = lat_query.shape[1] // KDIM
    rows, index_heads = index_weight.shape
    dims = index_keys.shape[1]
    factor = dims ** (-0.5)

    def swap(value, bits):
        return lax.ppermute(value, "seq", [(place, place ^ bits) for place in range(seq_count)])

    mine = jnp.concatenate([lat_keys.T, index_keys], axis=0)
    blocks = [mine] + [swap(mine, bits) for bits in range(2, seq_count, 2)]
    blocks = [block for even in blocks for block in (even, swap(even, 1))]

    offsets, scales, lows = spread(normalizer, index_weight, lookback, heads, factor)
    active, predicted, keys = index_scores(index_query, scales, lows, blocks, dims)
    own, *sends = attention_mass(lat_query, offsets, blocks, rows, peers)
    others = [
        lax.ppermute(send, "head", [(place, (place + hop + 1) % peers) for place in range(peers)])
        for hop, send in enumerate(sends)
    ]
    grad_query, grad_weight, key_terms = index_grads(
        own, others, predicted, active, scales, index_query, keys, factor
    )
    arrived = lax.all_to_all(key_terms, ("seq", "head"), 0, 0, tiled=True)
    grad_key = jnp.sum(
        arrived.reshape(seq_count * peers, -1, dims).astype(jnp.float32), axis=0
    )
    return grad_query, grad_weight, grad_key


def solution(mesh):
    return jax.shard_map(
        per_device,
        mesh=mesh,
        in_specs=(
            P("seq", "head"),
            P("seq", None),
            P("seq", None),
            P("seq"),
            P(("seq", "head"), None),
            P("seq", None),
            P(("seq", "head"), None),
        ),
        out_specs=(P(("seq", "head"), None), P(("seq", "head"), None), P(("seq", "head"), None)),
        check_vma=False,
    )
```

```python
import functools
import math

import jax
import jax.numpy as jnp
from jax import lax
from jax.experimental import pallas as pl
from jax.experimental.pallas import tpu as pltpu
from jax.sharding import PartitionSpec as P


KDIM = 576
LANES = 128
WIDE = 2 * LANES
PAD = LANES - KDIM % LANES
LOG2E = 1.0 / math.log(2.0)
HBM = pl.BlockSpec(memory_space=pltpu.HBM)
VMEM = pl.BlockSpec(memory_space=pltpu.VMEM)


def shape_of(dims, kind):
    return jax.ShapeDtypeStruct(dims, kind)


def call(body, out_shape, args, specs=None, scratch=(), flops=0, limit=20):
    return pl.pallas_call(
        body,
        out_shape=out_shape,
        in_specs=specs or [VMEM] * len(args),
        out_specs=jax.tree.map(lambda _: VMEM, out_shape),
        scratch_shapes=list(scratch),
        compiler_params=pltpu.CompilerParams(vmem_limit_bytes=limit << 20),
        cost_estimate=pl.CostEstimate(flops=flops, bytes_accessed=0, transcendentals=0),
    )(*args)


def lanes_of(place):
    return slice(place * LANES, (place + 1) * LANES)


def spread_kernel(factor, query_hbm, norm_hbm, weight_hbm, look_hbm, *refs):
    query_ref, off_ref, scale_ref, low_ref, norm, weight, look, tall, sems = refs
    pairs = ((norm_hbm, norm), (weight_hbm, weight), (look_hbm, look), (query_hbm, query_ref))
    copies = [pltpu.make_async_copy(*pair, sems.at[place]) for place, pair in enumerate(pairs)]
    for copy in copies:
        copy.start()
    heads, local_rows, _ = off_ref.shape
    rows = low_ref.shape[0]
    me = lax.axis_index("head")
    copies[0].wait()
    width = norm.shape[1]
    offsets = pltpu.roll(norm[...] * LOG2E, lax.rem(width - me * heads, width), 1)
    for head in range(heads):
        off_ref[head] = jnp.broadcast_to(offsets[:, head : head + 1], (local_rows, LANES))
    copies[1].wait()
    weights = weight[...] * factor
    for head in range(scale_ref.shape[0]):
        scale_ref[head] = jnp.broadcast_to(weights[:, head : head + 1], (rows, LANES))
    copies[2].wait()
    tall[...] = jnp.transpose(
        jnp.broadcast_to(look[...].astype(jnp.float32), (LANES, local_rows))
    )
    low_ref[...] = tall[pl.ds(me * rows, rows), :]
    copies[3].wait()


def spread(lat_query, normalizer, weight, lookback, heads, factor):
    rows, index_heads = weight.shape
    local_rows = normalizer.shape[0]
    look = lookback.reshape(1, local_rows)
    out = (
        shape_of(lat_query.shape, lat_query.dtype),
        shape_of((heads, local_rows, LANES), jnp.float32),
        shape_of((index_heads, rows, LANES), jnp.float32),
        shape_of((rows, LANES), jnp.float32),
    )
    scratch = [pltpu.VMEM(value.shape, value.dtype) for value in (normalizer, weight, look)]
    scratch += [pltpu.VMEM((local_rows, LANES), jnp.float32), pltpu.SemaphoreType.DMA((4,))]
    return call(
        functools.partial(spread_kernel, factor),
        out,
        tuple(pltpu.with_memory_space_constraint(value, pltpu.HBM) for value in (lat_query, normalizer, weight, look)),
        specs=[HBM] * 4,
        scratch=scratch,
        flops=1_500_000_000,
    )


def mass_kernel(slots, carried, places, query_ref, off_ref, *refs):
    blocks, refs = refs[:slots], refs[slots:]
    prior, refs = refs[:carried], refs[carried:]
    outs, (keys, acc) = refs[:-2], refs[-2:]
    tiles, local_rows, wide = acc.shape
    heads = off_ref.shape[0]
    group = min(16, heads)
    depth = KDIM + PAD
    per_tile = wide // LANES
    for tile in range(tiles):
        keys[tile, :PAD] = jnp.zeros((PAD, wide), keys.dtype)
        keys[tile, PAD + KDIM :] = jnp.zeros((PAD, wide), keys.dtype)
        for part in range(per_tile):
            keys[tile, PAD : PAD + KDIM, lanes_of(part)] = blocks[tile * per_tile + part][:KDIM]
    acc[...] = jnp.zeros_like(acc)
    scale = KDIM ** (-0.5) * LOG2E

    @pl.loop(0, heads // group)
    def _(step):
        @pl.loop(0, tiles)
        def _(tile):
            total = acc[tile]
            for odd in range(2):
                picked = []
                for head in range(odd, group, 2):
                    begin = step * (group * KDIM) + (head * KDIM - (PAD if odd else 0))
                    picked.append(query_ref[:, pl.ds(pl.multiple_of(begin, LANES), depth)])
                first = 0 if odd else PAD
                scores = jnp.dot(
                    jnp.concatenate(picked, axis=0),
                    keys[tile, first : first + depth],
                    preferred_element_type=jnp.float32,
                )
                for place, head in enumerate(range(odd, group, 2)):
                    offset = jnp.concatenate([off_ref[step * group + head]] * per_tile, axis=1)
                    part = scores[place * local_rows : (place + 1) * local_rows]
                    total = total + jnp.exp2(part * scale - offset)
            acc[tile] = total

    if not places:
        outs[0][...] = acc[...]
        return
    own, sends = outs[0], outs[1:]
    rows = own.shape[0]
    size = len(sends) + 1
    me = lax.axis_index("head")
    sources = [(ref, tile) for ref in (*prior, acc) for tile in range(ref.shape[0])]
    pieces = [(ref, tile, part) for ref, tile in sources for part in range(per_tile)]
    for place, (ref, tile, part) in zip(places, pieces):
        lanes = lanes_of(part)
        own[:, lanes_of(place)] = ref[tile, pl.ds(me * rows, rows), lanes]
        for hop, send in enumerate(sends):
            there = lax.rem(me + hop + 1, size)
            send[:, lanes_of(place)] = ref[tile, pl.ds(there * rows, rows), lanes].astype(send.dtype)


def attention_mass(query, offsets, blocks, prior, places, rows, peers):
    local_rows = query.shape[0]
    heads = offsets.shape[0]
    slots = len(blocks)
    tiles = slots * LANES // WIDE
    if places:
        columns = len(places) * LANES
        out = (shape_of((rows, columns), jnp.float32),)
        out += (shape_of((rows, columns), jnp.bfloat16),) * (peers - 1)
    else:
        out = shape_of((tiles, local_rows, WIDE), jnp.float32)
    return call(
        functools.partial(mass_kernel, slots, len(prior), places),
        out,
        (query, offsets, *blocks, *prior),
        scratch=[
            pltpu.VMEM((tiles, KDIM + 2 * PAD, WIDE), jnp.bfloat16),
            pltpu.VMEM((tiles, local_rows, WIDE), jnp.float32),
        ],
        flops=2 * local_rows * heads * KDIM * slots * LANES,
    )


def stack_heads(value, heads, dims):
    parts = [value[:, head * dims : (head + 1) * dims] for head in range(heads)]
    if value.shape[0] % 16 == 0:
        return jnp.concatenate(parts, axis=0)
    parts = [part.astype(jnp.float32) for part in parts]
    return jnp.concatenate(parts, axis=0).astype(value.dtype)


def score_kernel(order, query_ref, scale_ref, low_ref, *refs):
    slots = len(order)
    blocks = refs[:slots]
    active_ref, predicted_ref, keys, score = refs[slots:]
    index_heads, rows, seq_total = active_ref.shape
    dims = keys.shape[1]
    group = min(8, index_heads)
    score[...] = jnp.zeros_like(score)
    for place in range(slots):
        keys[lanes_of(place)] = blocks[place][KDIM:]

    @pl.loop(0, index_heads // group)
    def _(step):
        begin = pl.multiple_of(step * (group * dims), LANES)
        stacked = stack_heads(query_ref[:, pl.ds(begin, group * dims)], group, dims)
        for begin in range(0, seq_total, WIDE):
            inner = lax.dot_general(
                stacked,
                keys[begin : begin + WIDE],
                (((1,), (1,)), ((), ())),
                preferred_element_type=jnp.float32,
            )
            total = score[:, begin : begin + WIDE]
            for head in range(group):
                active = jnp.maximum(inner[head * rows : (head + 1) * rows], 0.0)
                active_ref[step * group + head, :, begin : begin + WIDE] = active
                total = total + active * jnp.concatenate([scale_ref[step * group + head]] * 2, axis=1)
            score[:, begin : begin + WIDE] = total

    seq = lax.axis_index("seq")
    query_pos = (
        seq * lax.axis_size("head") + lax.axis_index("head")
    ) * rows + lax.broadcasted_iota(jnp.int32, (rows, LANES), 0)
    low = query_pos - low_ref[...].astype(jnp.int32)
    lane = lax.broadcasted_iota(jnp.int32, (rows, LANES), 1)
    seen = []
    for slot in order:
        key_pos = jnp.bitwise_xor(seq, slot) * LANES + lane
        seen.append((key_pos <= query_pos) & (key_pos >= low))
    parts = [score[:, lanes_of(place)] for place in range(slots)]
    parts = [jnp.where(see, part, -jnp.inf) for see, part in zip(seen, parts)]
    top = jnp.max(functools.reduce(jnp.maximum, parts), axis=1, keepdims=True)
    parts = [jnp.exp(part - top) for part in parts]
    mass = jnp.sum(functools.reduce(jnp.add, parts), axis=1, keepdims=True)
    for place in range(slots):
        predicted_ref[:, lanes_of(place)] = jnp.where(seen[place], parts[place] / mass, -1.0)


def index_scores(index_query, scales, lows, blocks, order, dims):
    rows = index_query.shape[0]
    index_heads = scales.shape[0]
    seq_total = len(order) * LANES
    return call(
        functools.partial(score_kernel, order),
        (
            shape_of((index_heads, rows, seq_total), jnp.float32),
            shape_of((rows, seq_total), jnp.float32),
            shape_of((seq_total, dims), jnp.bfloat16),
        ),
        (index_query, scales, lows, *blocks),
        scratch=[pltpu.VMEM((rows, seq_total), jnp.float32)],
        flops=6 * rows * index_heads * seq_total * dims,
    )


def gap_of(shares, predicted):
    mine, *others = shares
    mass = mine[...]
    for other in others:
        mass = mass + other[...].astype(jnp.float32)
    seen = predicted >= 0.0
    mass = jnp.where(seen, mass, 0.0)
    target = mass / jnp.sum(mass, axis=1, keepdims=True)
    return jnp.where(seen, predicted - target, 0.0)


def key_kernel(peers, half, *refs):
    shares, refs = refs[:peers], refs[peers:]
    if peers:
        predicted_ref, active_ref, scale_ref, query_ref, gap_ref, slopes_ref, out_ref, tall = refs
        gap_ref[...] = gap_of(shares, predicted_ref[...])
    else:
        gap_ref, active_ref, scale_ref, query_ref, slopes_ref, out_ref, tall = refs
    index_heads, rows, _ = active_ref.shape
    dims, columns = tall.shape
    lanes = slice(half * columns, (half + 1) * columns)
    group = min(8, index_heads)
    tall[...] = jnp.zeros_like(tall)

    @pl.loop(0, index_heads // group)
    def _(step):
        gap = gap_ref[:, lanes]
        slopes = []
        for head in range(group):
            place = step * group + head
            scaled = gap * jnp.concatenate([scale_ref[place]] * (columns // LANES), axis=1)
            slope = jnp.where(active_ref[place, :, lanes] > 0.0, scaled, 0.0)
            slopes.append(slope if rows % 16 else slope.astype(jnp.bfloat16))
        slopes = jnp.concatenate(slopes, axis=0).astype(jnp.bfloat16)
        block = pl.ds(pl.multiple_of(step * (group * rows), group * rows), group * rows)
        slopes_ref[block, :] = slopes
        begin = pl.multiple_of(step * (group * dims), LANES)
        stacked = stack_heads(query_ref[:, pl.ds(begin, group * dims)], group, dims)
        tall[...] += lax.dot_general(
            stacked, slopes, (((0,), (0,)), ((), ())), preferred_element_type=jnp.float32
        )

    for place in range(columns // LANES):
        out_ref[lanes_of(place)] = jnp.transpose(tall[:, lanes_of(place)])


def key_terms(shares, gap, predicted, active, scales, index_query, dims, half):
    index_heads, rows, seq_total = active.shape
    columns = seq_total // 2
    out = (
        shape_of((index_heads * rows, columns), jnp.bfloat16),
        shape_of((columns, dims), jnp.float32),
    )
    if shares:
        out = (shape_of((rows, seq_total), jnp.float32), *out)
        args = (*shares, predicted)
    else:
        args = (gap,)
    return call(
        functools.partial(key_kernel, len(shares), half),
        out,
        (*args, active, scales, index_query),
        scratch=[pltpu.VMEM((dims, columns), jnp.float32)],
        flops=4 * rows * index_heads * seq_total * dims,
    )


def query_kernel(factor, gap_ref, even_ref, odd_ref, active_ref, keys_ref, grad_query_ref, grad_weight_ref, sums):
    index_heads, rows, seq_total = active_ref.shape
    dims = keys_ref.shape[1]
    group = min(8, index_heads)
    lane = lax.broadcasted_iota(jnp.int32, (rows, LANES), 1)
    sums[...] = jnp.zeros_like(sums)

    @pl.loop(0, index_heads // group)
    def _(step):
        gap = gap_ref[...]
        total = sums[...]
        for head in range(group):
            product = active_ref[step * group + head] * gap
            partial = functools.reduce(
                jnp.add, [product[:, lanes_of(place)] for place in range(seq_total // LANES)]
            )
            partial = jnp.sum(partial, axis=1, keepdims=True)
            total = jnp.where(lane == step * group + head, partial, total)
        sums[...] = total
        block = pl.ds(pl.multiple_of(step * (group * rows), group * rows), group * rows)
        slopes = jnp.concatenate([even_ref[block, :], odd_ref[block, :]], axis=1)
        grad = jnp.dot(slopes, keys_ref[...], preferred_element_type=jnp.float32)
        for head in range(group):
            begin = pl.multiple_of((step * group + head) * dims, dims)
            grad_query_ref[:, pl.ds(begin, dims)] = grad[head * rows : (head + 1) * rows]

    grad_weight_ref[...] = sums[:, :index_heads] * factor


def query_grads(gap, even, odd, active, keys, factor):
    index_heads, rows, seq_total = active.shape
    dims = keys.shape[1]
    return call(
        functools.partial(query_kernel, factor),
        (
            shape_of((rows, index_heads * dims), jnp.float32),
            shape_of((rows, index_heads), jnp.float32),
        ),
        (gap, even, odd, active, keys),
        scratch=[pltpu.VMEM((rows, LANES), jnp.float32)],
        flops=6 * rows * index_heads * seq_total * dims,
    )


def fold_kernel(keep_ref, come_ref, own_ref, *sends):
    total = keep_ref[...] + come_ref[...]
    rows = own_ref.shape[0]
    own_ref[...] = total[:rows]
    for hop, send in enumerate(sends):
        send[...] = total[(hop + 1) * rows : (hop + 2) * rows].astype(send.dtype)


def fold(keep, come, block):
    count = keep.shape[0] // block
    piece = (block, keep.shape[1])
    out = (shape_of(piece, jnp.float32),) + (shape_of(piece, jnp.bfloat16),) * (count - 1)
    return call(fold_kernel, out, (keep, come), flops=10_000_000)


def per_device(lat_query, lat_keys, normalizer, lookback, index_query, index_keys, index_weight):
    seq_count = lax.axis_size("seq")
    peers = lax.axis_size("head")
    heads = lat_query.shape[1] // KDIM
    rows, _ = index_weight.shape
    dims = index_keys.shape[1]
    factor = dims ** (-0.5)

    def swap(value, bits):
        return lax.ppermute(value, "seq", [(place, place ^ bits) for place in range(seq_count)])

    def pass_on(values):
        out = []
        for hop, value in enumerate(values):
            to = [(place, (place + hop + 1) % peers) for place in range(peers)]
            out.append(lax.ppermute(value, "head", to))
        return out

    mine = jnp.concatenate([lat_keys.T, index_keys], axis=0)
    blocks = {0: mine}
    for bits in range(2, seq_count, 2):
        blocks[bits] = swap(mine, bits)
    for bits in range(0, seq_count, 2):
        blocks[bits + 1] = swap(blocks[bits], 1)
    phases = [[0, 1], [2, 4], [3, 5], list(range(6, seq_count))]
    order = [*range(0, seq_count, 2), *range(1, seq_count, 2)]

    query, offsets, scales, lows = spread(
        lat_query, normalizer, index_weight, lookback, heads, factor
    )
    prior = []
    for phase in phases:
        last = phase is phases[-1]
        mass = attention_mass(
            query,
            offsets,
            [blocks[slot] for slot in phase],
            prior if last else [],
            [order.index(slot) for slots in phases for slot in slots] if last else [],
            rows,
            peers,
        )
        prior.append(mass)
    own, *sends = mass
    shares = [own, *pass_on(sends)]
    active, predicted, keys = index_scores(
        index_query, scales, lows, [blocks[slot] for slot in order], order, dims
    )
    terms = functools.partial(
        key_terms, active=active, scales=scales, index_query=index_query, dims=dims
    )
    gap, odd, give = terms(shares, None, predicted, half=1)
    come = swap(give, 1)
    even, keep = terms([], gap, None, half=0)
    own, *sends = fold(keep, come, LANES)
    others = [swap(send, 2 * (hop + 1)) for hop, send in enumerate(sends)]
    grad_query, grad_weight = query_grads(gap, even, odd, active, keys, factor)
    own, *sends = gather_terms(own, others, rows, peers)
    others = pass_on(sends)
    grad_key = functools.reduce(jnp.add, others, own)
    return grad_query, grad_weight, grad_key


def gather_kernel(peers, own_ref, *refs):
    others, (mine_ref, *sends), total = refs[: len(refs) - peers - 1], refs[-peers - 1 : -1], refs[-1]
    value = own_ref[...]
    for other in others:
        value = value + other[...].astype(jnp.float32)
    total[...] = value
    rows = mine_ref.shape[0]
    me = lax.axis_index("head")
    mine_ref[...] = total[pl.ds(me * rows, rows), :]
    for hop, send in enumerate(sends):
        send[...] = total[pl.ds(lax.rem(me + hop + 1, peers) * rows, rows), :]


def gather_terms(own, others, rows, peers):
    piece = shape_of((rows, own.shape[1]), jnp.float32)
    return call(
        functools.partial(gather_kernel, peers),
        (piece,) * peers,
        (own, *others),
        scratch=[pltpu.VMEM(own.shape, jnp.float32)],
        flops=10_000_000,
    )


def solution(mesh):
    return jax.shard_map(
        per_device,
        mesh=mesh,
        in_specs=(
            P("seq", "head"),
            P("seq", None),
            P("seq", None),
            P("seq"),
            P(("seq", "head"), None),
            P("seq", None),
            P(("seq", "head"), None),
        ),
        out_specs=(P(("seq", "head"), None), P(("seq", "head"), None), P(("seq", "head"), None)),
        check_vma=False,
    )
```

```python
import functools
import math

import jax
import jax.numpy as jnp
from jax import lax
from jax.experimental import pallas as pl
from jax.experimental.pallas import tpu as pltpu
from jax.sharding import PartitionSpec as P


KDIM = 576
LANES = 128
WIDE = 2 * LANES
PAD = LANES - KDIM % LANES
LOG2E = 1.0 / math.log(2.0)
HBM = pl.BlockSpec(memory_space=pltpu.HBM)
VMEM = pl.BlockSpec(memory_space=pltpu.VMEM)


def shape_of(dims, kind):
    return jax.ShapeDtypeStruct(dims, kind)


def call(body, out_shape, args, specs=None, scratch=(), flops=0, limit=20):
    return pl.pallas_call(
        body,
        out_shape=out_shape,
        in_specs=specs or [VMEM] * len(args),
        out_specs=jax.tree.map(lambda _: VMEM, out_shape),
        scratch_shapes=list(scratch),
        compiler_params=pltpu.CompilerParams(vmem_limit_bytes=limit << 20),
        cost_estimate=pl.CostEstimate(flops=flops, bytes_accessed=0, transcendentals=0),
    )(*args)


def lanes_of(place):
    return slice(place * LANES, (place + 1) * LANES)


def spread_kernel(factor, query_hbm, norm_hbm, weight_hbm, look_hbm, *refs):
    query_ref, off_ref, scale_ref, low_ref, norm, weight, look, tall, sems = refs
    pairs = ((norm_hbm, norm), (weight_hbm, weight), (look_hbm, look), (query_hbm, query_ref))
    copies = [pltpu.make_async_copy(*pair, sems.at[place]) for place, pair in enumerate(pairs)]
    for copy in copies:
        copy.start()
    heads, local_rows, _ = off_ref.shape
    rows = low_ref.shape[0]
    me = lax.axis_index("head")
    copies[0].wait()
    width = norm.shape[1]
    offsets = pltpu.roll(norm[...] * LOG2E, lax.rem(width - me * heads, width), 1)
    for head in range(heads):
        off_ref[head] = jnp.broadcast_to(offsets[:, head : head + 1], (local_rows, LANES))
    copies[1].wait()
    weights = weight[...] * factor
    for head in range(scale_ref.shape[0]):
        scale_ref[head] = jnp.broadcast_to(weights[:, head : head + 1], (rows, LANES))
    copies[2].wait()
    tall[...] = jnp.transpose(
        jnp.broadcast_to(look[...].astype(jnp.float32), (LANES, local_rows))
    )
    low_ref[...] = tall[pl.ds(me * rows, rows), :]
    copies[3].wait()


def spread(lat_query, normalizer, weight, lookback, heads, factor):
    rows, index_heads = weight.shape
    local_rows = normalizer.shape[0]
    look = lookback.reshape(1, local_rows)
    out = (
        shape_of(lat_query.shape, lat_query.dtype),
        shape_of((heads, local_rows, LANES), jnp.float32),
        shape_of((index_heads, rows, LANES), jnp.float32),
        shape_of((rows, LANES), jnp.float32),
    )
    scratch = [pltpu.VMEM(value.shape, value.dtype) for value in (normalizer, weight, look)]
    scratch += [pltpu.VMEM((local_rows, LANES), jnp.float32), pltpu.SemaphoreType.DMA((4,))]
    return call(
        functools.partial(spread_kernel, factor),
        out,
        tuple(pltpu.with_memory_space_constraint(value, pltpu.HBM) for value in (lat_query, normalizer, weight, look)),
        specs=[HBM] * 4,
        scratch=scratch,
        flops=1_500_000_000,
    )


def mass_kernel(slots, carried, places, query_ref, off_ref, *refs):
    blocks, refs = refs[:slots], refs[slots:]
    prior, refs = refs[:carried], refs[carried:]
    outs, (keys, acc) = refs[:-2], refs[-2:]
    tiles, local_rows, wide = acc.shape
    heads = off_ref.shape[0]
    group = min(16, heads)
    depth = KDIM + PAD
    per_tile = wide // LANES
    for tile in range(tiles):
        keys[tile, :PAD] = jnp.zeros((PAD, wide), keys.dtype)
        keys[tile, PAD + KDIM :] = jnp.zeros((PAD, wide), keys.dtype)
        for part in range(per_tile):
            keys[tile, PAD : PAD + KDIM, lanes_of(part)] = blocks[tile * per_tile + part][:KDIM]
    acc[...] = jnp.zeros_like(acc)
    scale = KDIM ** (-0.5) * LOG2E

    @pl.loop(0, heads // group)
    def _(step):
        @pl.loop(0, tiles)
        def _(tile):
            total = acc[tile]
            for odd in range(2):
                picked = []
                for head in range(odd, group, 2):
                    begin = step * (group * KDIM) + (head * KDIM - (PAD if odd else 0))
                    picked.append(query_ref[:, pl.ds(pl.multiple_of(begin, LANES), depth)])
                first = 0 if odd else PAD
                scores = jnp.dot(
                    jnp.concatenate(picked, axis=0),
                    keys[tile, first : first + depth],
                    preferred_element_type=jnp.float32,
                )
                for place, head in enumerate(range(odd, group, 2)):
                    offset = jnp.concatenate([off_ref[step * group + head]] * per_tile, axis=1)
                    part = scores[place * local_rows : (place + 1) * local_rows]
                    total = total + jnp.exp2(part * scale - offset)
            acc[tile] = total

    if not places:
        outs[0][...] = acc[...]
        return
    own, sends = outs[0], outs[1:]
    rows = own.shape[0]
    me = lax.axis_index("head")
    sources = [(ref, tile) for ref in (*prior, acc) for tile in range(ref.shape[0])]
    pieces = [(ref, tile, part) for ref, tile in sources for part in range(per_tile)]
    for place, (ref, tile, part) in zip(places, pieces):
        lanes = lanes_of(part)
        own[:, lanes_of(place)] = ref[tile, pl.ds(me * rows, rows), lanes]
        for hop, send in enumerate(sends):
            there = jnp.bitwise_xor(me, hop + 1)
            send[:, lanes_of(place)] = ref[tile, pl.ds(there * rows, rows), lanes].astype(send.dtype)


def attention_mass(query, offsets, blocks, prior, places, rows, peers):
    local_rows = query.shape[0]
    heads = offsets.shape[0]
    slots = len(blocks)
    tiles = slots * LANES // WIDE
    if places:
        columns = len(places) * LANES
        out = (shape_of((rows, columns), jnp.float32),)
        out += (shape_of((rows, columns), jnp.bfloat16),) * (peers - 1)
    else:
        out = shape_of((tiles, local_rows, WIDE), jnp.float32)
    return call(
        functools.partial(mass_kernel, slots, len(prior), places),
        out,
        (query, offsets, *blocks, *prior),
        scratch=[
            pltpu.VMEM((tiles, KDIM + 2 * PAD, WIDE), jnp.bfloat16),
            pltpu.VMEM((tiles, local_rows, WIDE), jnp.float32),
        ],
        flops=2 * local_rows * heads * KDIM * slots * LANES,
    )


def stack_heads(value, heads, dims):
    parts = [value[:, head * dims : (head + 1) * dims] for head in range(heads)]
    if value.shape[0] % 16 == 0:
        return jnp.concatenate(parts, axis=0)
    parts = [part.astype(jnp.float32) for part in parts]
    return jnp.concatenate(parts, axis=0).astype(value.dtype)


def score_kernel(slots, query_ref, scale_ref, *refs):
    blocks, (active_ref, score, keys) = refs[:slots], refs[slots:]
    score_blocks(blocks, query_ref, scale_ref, active_ref, score, keys)


def score_blocks(blocks, query_ref, scale_ref, active_ref, score, keys):
    index_heads, rows, columns = active_ref.shape
    dims = keys.shape[1]
    group = min(8, index_heads)
    score[...] = jnp.zeros_like(score)
    for place, block in enumerate(blocks):
        keys[lanes_of(place)] = block[KDIM:]

    @pl.loop(0, index_heads // group)
    def _(step):
        begin = pl.multiple_of(step * (group * dims), LANES)
        stacked = stack_heads(query_ref[:, pl.ds(begin, group * dims)], group, dims)
        for begin in range(0, columns, WIDE):
            inner = lax.dot_general(
                stacked,
                keys[begin : begin + WIDE],
                (((1,), (1,)), ((), ())),
                preferred_element_type=jnp.float32,
            )
            total = score[:, begin : begin + WIDE]
            for head in range(group):
                active = jnp.maximum(inner[head * rows : (head + 1) * rows], 0.0)
                active_ref[step * group + head, :, begin : begin + WIDE] = active
                total = total + active * jnp.concatenate([scale_ref[step * group + head]] * 2, axis=1)
            score[:, begin : begin + WIDE] = total


def predict_kernel(order, slots, query_ref, scale_ref, low_ref, first_ref, first_keys_ref, *refs):
    blocks, refs = refs[:slots], refs[slots:]
    active_ref, predicted_ref, keys_ref, score, keys = refs
    score_blocks(blocks, query_ref, scale_ref, active_ref, score, keys)
    rows = score.shape[0]
    halves = halved((first_ref, score), 1)
    for half in range(2):
        begin = half * (len(order) // 2) * LANES
        for ref in (first_keys_ref, keys):
            part = ref.shape[0] // 2
            keys_ref[begin : begin + part] = ref[half * part : (half + 1) * part]
            begin += part

    seq = lax.axis_index("seq")
    query_pos = (
        seq * lax.axis_size("head") + lax.axis_index("head")
    ) * rows + lax.broadcasted_iota(jnp.int32, (rows, LANES), 0)
    low = query_pos - low_ref[...].astype(jnp.int32)
    lane = lax.broadcasted_iota(jnp.int32, (rows, LANES), 1)
    scores = jnp.concatenate(halves, axis=1)
    parts, seen = [], []
    for place, slot in enumerate(order):
        key_pos = jnp.bitwise_xor(seq, slot) * LANES + lane
        seen.append((key_pos <= query_pos) & (key_pos >= low))
        parts.append(jnp.where(seen[-1], scores[:, lanes_of(place)], -jnp.inf))
    top = jnp.max(functools.reduce(jnp.maximum, parts), axis=1, keepdims=True)
    parts = [jnp.exp(part - top) for part in parts]
    mass = jnp.sum(functools.reduce(jnp.add, parts), axis=1, keepdims=True)
    for place in range(len(order)):
        predicted_ref[:, lanes_of(place)] = jnp.where(seen[place], parts[place] / mass, -1.0)


def halved(refs, axis, *index):
    out = []
    for half in range(2):
        parts = []
        for ref in refs:
            part = ref.shape[-1] // 2
            parts.append(ref[(*index, slice(None), slice(half * part, (half + 1) * part))])
        out.append(jnp.concatenate(parts, axis=axis))
    return out


def index_scores(index_query, scales, blocks, dims):
    rows = index_query.shape[0]
    index_heads = scales.shape[0]
    columns = len(blocks) * LANES
    return call(
        functools.partial(score_kernel, len(blocks)),
        (
            shape_of((index_heads, rows, columns), jnp.float32),
            shape_of((rows, columns), jnp.float32),
            shape_of((columns, dims), jnp.bfloat16),
        ),
        (index_query, scales, *blocks),
        flops=6 * rows * index_heads * columns * dims,
    )


def predictions(index_query, scales, lows, scores, keys, blocks, order, dims):
    rows = index_query.shape[0]
    index_heads = scales.shape[0]
    columns = len(blocks) * LANES
    seq_total = len(order) * LANES
    return call(
        functools.partial(predict_kernel, order, len(blocks)),
        (
            shape_of((index_heads, rows, columns), jnp.float32),
            shape_of((rows, seq_total), jnp.float32),
            shape_of((seq_total, dims), jnp.bfloat16),
        ),
        (index_query, scales, lows, scores, keys, *blocks),
        scratch=[
            pltpu.VMEM((rows, columns), jnp.float32),
            pltpu.VMEM((columns, dims), jnp.bfloat16),
        ],
        flops=8 * rows * index_heads * columns * dims,
    )


def gap_of(shares, predicted):
    mine, *others = shares
    mass = mine[...]
    for other in others:
        mass = mass + other[...].astype(jnp.float32)
    seen = predicted >= 0.0
    mass = jnp.where(seen, mass, 0.0)
    target = mass / jnp.sum(mass, axis=1, keepdims=True)
    return jnp.where(seen, predicted - target, 0.0)


def key_kernel(peers, half, *refs):
    shares, refs = refs[:peers], refs[peers:]
    if peers:
        predicted_ref, *actives, scale_ref, query_ref, gap_ref, slopes_ref, out_ref, tall = refs
        gap_ref[...] = gap_of(shares, predicted_ref[...])
    else:
        gap_ref, *actives, scale_ref, query_ref, slopes_ref, out_ref, tall = refs
    index_heads, rows, _ = actives[0].shape
    dims, columns = tall.shape
    lanes = slice(half * columns, (half + 1) * columns)
    group = min(8, index_heads)
    tall[...] = jnp.zeros_like(tall)

    @pl.loop(0, index_heads // group)
    def _(step):
        gap = gap_ref[:, lanes]
        slopes = []
        for head in range(group):
            place = step * group + head
            scaled = gap * jnp.concatenate([scale_ref[place]] * (columns // LANES), axis=1)
            slope = jnp.where(halved(actives, 1, place)[half] > 0.0, scaled, 0.0)
            slopes.append(slope if rows % 16 else slope.astype(jnp.bfloat16))
        slopes = jnp.concatenate(slopes, axis=0).astype(jnp.bfloat16)
        block = pl.ds(pl.multiple_of(step * (group * rows), group * rows), group * rows)
        slopes_ref[block, :] = slopes
        begin = pl.multiple_of(step * (group * dims), LANES)
        stacked = stack_heads(query_ref[:, pl.ds(begin, group * dims)], group, dims)
        tall[...] += lax.dot_general(
            stacked, slopes, (((0,), (0,)), ((), ())), preferred_element_type=jnp.float32
        )

    for place in range(columns // LANES):
        out_ref[lanes_of(place)] = jnp.transpose(tall[:, lanes_of(place)])


def key_terms(shares, gap, predicted, actives, scales, index_query, dims, half):
    index_heads, rows, _ = actives[0].shape
    seq_total = sum(active.shape[2] for active in actives)
    columns = seq_total // 2
    out = (
        shape_of((index_heads * rows, columns), jnp.bfloat16),
        shape_of((columns, dims), jnp.float32),
    )
    if shares:
        out = (shape_of((rows, seq_total), jnp.float32), *out)
        args = (*shares, predicted)
    else:
        args = (gap,)
    return call(
        functools.partial(key_kernel, len(shares), half),
        out,
        (*args, *actives, scales, index_query),
        scratch=[pltpu.VMEM((dims, columns), jnp.float32)],
        flops=4 * rows * index_heads * seq_total * dims,
    )


def query_kernel(even_ref, odd_ref, keys_ref, grad_query_ref):
    rows = grad_query_ref.shape[0]
    dims = keys_ref.shape[1]
    index_heads = grad_query_ref.shape[1] // dims
    group = min(8, index_heads)

    @pl.loop(0, index_heads // group)
    def _(step):
        block = pl.ds(pl.multiple_of(step * (group * rows), group * rows), group * rows)
        slopes = jnp.concatenate([even_ref[block, :], odd_ref[block, :]], axis=1)
        grad = jnp.dot(slopes, keys_ref[...], preferred_element_type=jnp.float32)
        for head in range(group):
            begin = pl.multiple_of((step * group + head) * dims, dims)
            grad_query_ref[:, pl.ds(begin, dims)] = grad[head * rows : (head + 1) * rows]


def query_grads(even, odd, keys, rows):
    return call(
        query_kernel,
        shape_of((rows, even.shape[0] // rows * keys.shape[1]), jnp.float32),
        (even, odd, keys),
        flops=4 * even.shape[0] * keys.shape[0] * keys.shape[1],
    )


def weight_kernel(factor, gap_ref, *refs):
    *actives, grad_weight_ref, sums = refs
    index_heads, rows, _ = actives[0].shape
    group = min(8, index_heads)
    lane = lax.broadcasted_iota(jnp.int32, (rows, LANES), 1)
    sums[...] = jnp.zeros_like(sums)

    @pl.loop(0, index_heads // group)
    def _(step):
        gap = gap_ref[...]
        total = sums[...]
        for head in range(group):
            place = step * group + head
            product = jnp.concatenate(halved(actives, 1, place), axis=1) * gap
            partial = functools.reduce(
                jnp.add, [product[:, lanes_of(slot)] for slot in range(gap.shape[1] // LANES)]
            )
            partial = jnp.sum(partial, axis=1, keepdims=True)
            total = jnp.where(lane == place, partial, total)
        sums[...] = total

    grad_weight_ref[...] = sums[:, :index_heads] * factor


def weight_grads(gap, actives, factor):
    index_heads, rows, _ = actives[0].shape
    return call(
        functools.partial(weight_kernel, factor),
        shape_of((rows, index_heads), jnp.float32),
        (gap, *actives),
        scratch=[pltpu.VMEM((rows, LANES), jnp.float32)],
        flops=512 * rows * index_heads * gap.shape[1],
    )


def fold_kernel(keep_ref, come_ref, own_ref, *sends):
    total = keep_ref[...] + come_ref[...]
    rows = own_ref.shape[0]
    own_ref[...] = total[:rows]
    for hop, send in enumerate(sends):
        send[...] = total[(hop + 1) * rows : (hop + 2) * rows].astype(send.dtype)


def fold(keep, come, block):
    count = keep.shape[0] // block
    piece = (block, keep.shape[1])
    out = (shape_of(piece, jnp.float32),) + (shape_of(piece, jnp.bfloat16),) * (count - 1)
    return call(fold_kernel, out, (keep, come), flops=10_000_000)


def per_device(lat_query, lat_keys, normalizer, lookback, index_query, index_keys, index_weight):
    seq_count = lax.axis_size("seq")
    peers = lax.axis_size("head")
    heads = lat_query.shape[1] // KDIM
    rows, _ = index_weight.shape
    dims = index_keys.shape[1]
    factor = dims ** (-0.5)

    def swap(value, bits):
        return lax.ppermute(value, "seq", [(place, place ^ bits) for place in range(seq_count)])

    def pass_on(values):
        out = []
        for hop, value in enumerate(values):
            to = [(place, place ^ (hop + 1)) for place in range(peers)]
            out.append(lax.ppermute(value, "head", to))
        return out

    mine = jnp.concatenate([lat_keys.T, index_keys], axis=0)
    blocks = {0: mine}
    for bits in range(2, seq_count, 2):
        blocks[bits] = swap(mine, bits)
    for bits in range(0, seq_count, 2):
        blocks[bits + 1] = swap(blocks[bits], 1)
    phases = [[0, 1], [2, 4], [3, 5], list(range(6, seq_count))]
    order = [*range(0, seq_count, 2), *range(1, seq_count, 2)]

    query, offsets, scales, lows = spread(
        lat_query, normalizer, index_weight, lookback, heads, factor
    )
    prior = []
    for phase in phases:
        last = phase is phases[-1]
        mass = attention_mass(
            query,
            offsets,
            [blocks[slot] for slot in phase],
            prior if last else [],
            [order.index(slot) for slots in phases for slot in slots] if last else [],
            rows,
            peers,
        )
        prior.append(mass)
    own, *sends = mass
    shares = [own, *pass_on(sends)]
    early = sorted((slot for phase in phases[:-1] for slot in phase), key=order.index)
    late = sorted(phases[-1], key=order.index)
    first, scores, keys = index_scores(index_query, scales, [blocks[slot] for slot in early], dims)
    second, predicted, keys = predictions(
        index_query, scales, lows, scores, keys, [blocks[slot] for slot in late], order, dims
    )
    terms = functools.partial(
        key_terms, actives=(first, second), scales=scales, index_query=index_query, dims=dims
    )
    gap, odd, give = terms(shares, None, predicted, half=1)
    come = swap(give, 1)
    even, keep = terms([], gap, None, half=0)
    own, *sends = fold(keep, come, LANES)
    others = [swap(send, 2 * (hop + 1)) for hop, send in enumerate(sends)]
    grad_query = query_grads(even, odd, keys, rows)
    grad_weight = weight_grads(gap, (first, second), factor)
    own, *sends = gather_terms(own, others, rows, peers)
    others = pass_on(sends)
    grad_key = functools.reduce(jnp.add, others, own)
    return grad_query, grad_weight, grad_key


def gather_kernel(peers, own_ref, *refs):
    others, (mine_ref, *sends), total = refs[: len(refs) - peers - 1], refs[-peers - 1 : -1], refs[-1]
    value = own_ref[...]
    for other in others:
        value = value + other[...].astype(jnp.float32)
    total[...] = value
    rows = mine_ref.shape[0]
    me = lax.axis_index("head")
    mine_ref[...] = total[pl.ds(me * rows, rows), :]
    for hop, send in enumerate(sends):
        send[...] = total[pl.ds(jnp.bitwise_xor(me, hop + 1) * rows, rows), :]


def gather_terms(own, others, rows, peers):
    piece = shape_of((rows, own.shape[1]), jnp.float32)
    return call(
        functools.partial(gather_kernel, peers),
        (piece,) * peers,
        (own, *others),
        scratch=[pltpu.VMEM(own.shape, jnp.float32)],
        flops=10_000_000,
    )


def solution(mesh):
    return jax.shard_map(
        per_device,
        mesh=mesh,
        in_specs=(
            P("seq", "head"),
            P("seq", None),
            P("seq", None),
            P("seq"),
            P(("seq", "head"), None),
            P("seq", None),
            P(("seq", "head"), None),
        ),
        out_specs=(P(("seq", "head"), None), P(("seq", "head"), None), P(("seq", "head"), None)),
        check_vma=False,
    )
```

```python
import functools
import math

import jax
import jax.numpy as jnp
from jax import lax
from jax.experimental import pallas as pl
from jax.experimental.pallas import tpu as pltpu
from jax.sharding import PartitionSpec as P


KDIM = 576
LANES = 128
WIDE = 2 * LANES
PAD = LANES - KDIM % LANES
LOG2E = 1.0 / math.log(2.0)
HBM = pl.BlockSpec(memory_space=pltpu.HBM)
VMEM = pl.BlockSpec(memory_space=pltpu.VMEM)


def shape_of(dims, kind):
    return jax.ShapeDtypeStruct(dims, kind)


def call(body, out_shape, args, specs=None, scratch=(), flops=0, limit=20):
    return pl.pallas_call(
        body,
        out_shape=out_shape,
        in_specs=specs or [VMEM] * len(args),
        out_specs=jax.tree.map(lambda _: VMEM, out_shape),
        scratch_shapes=list(scratch),
        compiler_params=pltpu.CompilerParams(vmem_limit_bytes=limit << 20),
        cost_estimate=pl.CostEstimate(flops=flops, bytes_accessed=0, transcendentals=0),
    )(*args)


def lanes_of(place):
    return slice(place * LANES, (place + 1) * LANES)


def spread_kernel(factor, query_hbm, norm_hbm, weight_hbm, look_hbm, *refs):
    query_ref, off_ref, scale_ref, low_ref, norm, weight, look, tall, sems = refs
    pairs = ((norm_hbm, norm), (weight_hbm, weight), (look_hbm, look), (query_hbm, query_ref))
    copies = [pltpu.make_async_copy(*pair, sems.at[place]) for place, pair in enumerate(pairs)]
    for copy in copies:
        copy.start()
    heads, local_rows, _ = off_ref.shape
    rows = low_ref.shape[0]
    me = lax.axis_index("head")
    copies[0].wait()
    width = norm.shape[1]
    offsets = pltpu.roll(norm[...] * LOG2E, lax.rem(width - me * heads, width), 1)
    for head in range(heads):
        off_ref[head] = jnp.broadcast_to(offsets[:, head : head + 1], (local_rows, LANES))
    copies[1].wait()
    weights = weight[...] * factor
    for head in range(scale_ref.shape[0]):
        scale_ref[head] = jnp.broadcast_to(weights[:, head : head + 1], (rows, LANES))
    copies[2].wait()
    tall[...] = jnp.transpose(
        jnp.broadcast_to(look[...].astype(jnp.float32), (LANES, local_rows))
    )
    low_ref[...] = tall[pl.ds(me * rows, rows), :]
    copies[3].wait()


def spread(lat_query, normalizer, weight, lookback, heads, factor):
    rows, index_heads = weight.shape
    local_rows = normalizer.shape[0]
    look = lookback.reshape(1, local_rows)
    out = (
        shape_of(lat_query.shape, lat_query.dtype),
        shape_of((heads, local_rows, LANES), jnp.float32),
        shape_of((index_heads, rows, LANES), jnp.float32),
        shape_of((rows, LANES), jnp.float32),
    )
    scratch = [pltpu.VMEM(value.shape, value.dtype) for value in (normalizer, weight, look)]
    scratch += [pltpu.VMEM((local_rows, LANES), jnp.float32), pltpu.SemaphoreType.DMA((4,))]
    return call(
        functools.partial(spread_kernel, factor),
        out,
        tuple(pltpu.with_memory_space_constraint(value, pltpu.HBM) for value in (lat_query, normalizer, weight, look)),
        specs=[HBM] * 4,
        scratch=scratch,
        flops=1_500_000_000,
    )


def mass_kernel(slots, carried, places, query_ref, off_ref, *refs):
    blocks, refs = refs[:slots], refs[slots:]
    prior, refs = refs[:carried], refs[carried:]
    outs, (keys, acc) = refs[:-2], refs[-2:]
    tiles, local_rows, wide = acc.shape
    heads = off_ref.shape[0]
    group = min(32, heads)
    depth = KDIM + PAD
    per_tile = wide // LANES
    for tile in range(tiles):
        keys[tile, :PAD] = jnp.zeros((PAD, wide), keys.dtype)
        keys[tile, PAD + KDIM :] = jnp.zeros((PAD, wide), keys.dtype)
        for part in range(per_tile):
            keys[tile, PAD : PAD + KDIM, lanes_of(part)] = blocks[tile * per_tile + part][:KDIM]
    acc[...] = jnp.zeros_like(acc)
    scale = KDIM ** (-0.5) * LOG2E

    @pl.loop(0, heads // group)
    def _(step):
        @pl.loop(0, tiles)
        def _(tile):
            total = acc[tile]
            for odd in range(2):
                picked = []
                for head in range(odd, group, 2):
                    begin = step * (group * KDIM) + (head * KDIM - (PAD if odd else 0))
                    picked.append(query_ref[:, pl.ds(pl.multiple_of(begin, LANES), depth)])
                first = 0 if odd else PAD
                scores = jnp.dot(
                    jnp.concatenate(picked, axis=0),
                    keys[tile, first : first + depth],
                    preferred_element_type=jnp.float32,
                )
                for place, head in enumerate(range(odd, group, 2)):
                    offset = jnp.concatenate([off_ref[step * group + head]] * per_tile, axis=1)
                    part = scores[place * local_rows : (place + 1) * local_rows]
                    total = total + jnp.exp2(part * scale - offset)
            acc[tile] = total

    if not places:
        outs[0][...] = acc[...]
        return
    own, sends = outs[0], outs[1:]
    rows = own.shape[0]
    size = len(sends) + 1
    me = lax.axis_index("head")
    sources = [(ref, tile) for ref in (*prior, acc) for tile in range(ref.shape[0])]
    pieces = [(ref, tile, part) for ref, tile in sources for part in range(per_tile)]
    for place, (ref, tile, part) in zip(places, pieces):
        lanes = lanes_of(part)
        own[:, lanes_of(place)] = ref[tile, pl.ds(me * rows, rows), lanes]
        for hop, send in enumerate(sends):
            there = lax.rem(me + hop + 1, size)
            send[:, lanes_of(place)] = ref[tile, pl.ds(there * rows, rows), lanes].astype(send.dtype)


def attention_mass(query, offsets, blocks, prior, places, rows, peers):
    local_rows = query.shape[0]
    heads = offsets.shape[0]
    slots = len(blocks)
    tiles = slots * LANES // WIDE
    if places:
        columns = len(places) * LANES
        out = (shape_of((rows, columns), jnp.float32),)
        out += (shape_of((rows, columns), jnp.bfloat16),) * (peers - 1)
    else:
        out = shape_of((tiles, local_rows, WIDE), jnp.float32)
    return call(
        functools.partial(mass_kernel, slots, len(prior), places),
        out,
        (query, offsets, *blocks, *prior),
        scratch=[
            pltpu.VMEM((tiles, KDIM + 2 * PAD, WIDE), jnp.bfloat16),
            pltpu.VMEM((tiles, local_rows, WIDE), jnp.float32),
        ],
        flops=2 * local_rows * heads * KDIM * slots * LANES,
    )


def stack_heads(value, heads, dims):
    parts = [value[:, head * dims : (head + 1) * dims] for head in range(heads)]
    if value.shape[0] % 16 == 0:
        return jnp.concatenate(parts, axis=0)
    parts = [part.astype(jnp.float32) for part in parts]
    return jnp.concatenate(parts, axis=0).astype(value.dtype)


def score_kernel(order, query_ref, scale_ref, low_ref, *refs):
    slots = len(order)
    blocks = refs[:slots]
    active_ref, predicted_ref, keys, score = refs[slots:]
    index_heads, rows, seq_total = active_ref.shape
    dims = keys.shape[1]
    group = min(64, index_heads)
    score[...] = jnp.zeros_like(score)
    for place in range(slots):
        keys[lanes_of(place)] = blocks[place][KDIM:]

    @pl.loop(0, index_heads // group)
    def _(step):
        begin = pl.multiple_of(step * (group * dims), LANES)
        stacked = stack_heads(query_ref[:, pl.ds(begin, group * dims)], group, dims)
        for begin in range(0, seq_total, WIDE):
            inner = lax.dot_general(
                stacked,
                keys[begin : begin + WIDE],
                (((1,), (1,)), ((), ())),
                preferred_element_type=jnp.float32,
            )
            total = score[:, begin : begin + WIDE]
            for head in range(group):
                active = jnp.maximum(inner[head * rows : (head + 1) * rows], 0.0)
                active_ref[step * group + head, :, begin : begin + WIDE] = active
                total = total + active * jnp.concatenate([scale_ref[step * group + head]] * 2, axis=1)
            score[:, begin : begin + WIDE] = total

    seq = lax.axis_index("seq")
    query_pos = (
        seq * lax.axis_size("head") + lax.axis_index("head")
    ) * rows + lax.broadcasted_iota(jnp.int32, (rows, LANES), 0)
    low = query_pos - low_ref[...].astype(jnp.int32)
    lane = lax.broadcasted_iota(jnp.int32, (rows, LANES), 1)
    seen = []
    for slot in order:
        key_pos = jnp.bitwise_xor(seq, slot) * LANES + lane
        seen.append((key_pos <= query_pos) & (key_pos >= low))
    parts = [score[:, lanes_of(place)] for place in range(slots)]
    parts = [jnp.where(see, part, -jnp.inf) for see, part in zip(seen, parts)]
    top = jnp.max(functools.reduce(jnp.maximum, parts), axis=1, keepdims=True)
    parts = [jnp.exp(part - top) for part in parts]
    mass = jnp.sum(functools.reduce(jnp.add, parts), axis=1, keepdims=True)
    for place in range(slots):
        predicted_ref[:, lanes_of(place)] = jnp.where(seen[place], parts[place] / mass, -1.0)


def index_scores(index_query, scales, lows, blocks, order, dims):
    rows = index_query.shape[0]
    index_heads = scales.shape[0]
    seq_total = len(order) * LANES
    return call(
        functools.partial(score_kernel, order),
        (
            shape_of((index_heads, rows, seq_total), jnp.float32),
            shape_of((rows, seq_total), jnp.float32),
            shape_of((seq_total, dims), jnp.bfloat16),
        ),
        (index_query, scales, lows, *blocks),
        scratch=[pltpu.VMEM((rows, seq_total), jnp.float32)],
        flops=6 * rows * index_heads * seq_total * dims,
    )


def gap_of(shares, predicted):
    mine, *others = shares
    mass = mine[...]
    for other in others:
        mass = mass + other[...].astype(jnp.float32)
    seen = predicted >= 0.0
    mass = jnp.where(seen, mass, 0.0)
    target = mass / jnp.sum(mass, axis=1, keepdims=True)
    return jnp.where(seen, predicted - target, 0.0)


def key_kernel(peers, half, *refs):
    shares, refs = refs[:peers], refs[peers:]
    if peers:
        predicted_ref, active_ref, scale_ref, query_ref, gap_ref, slopes_ref, out_ref, tall = refs
        gap_ref[...] = gap_of(shares, predicted_ref[...])
    else:
        gap_ref, active_ref, scale_ref, query_ref, slopes_ref, out_ref, tall = refs
    index_heads, rows, _ = active_ref.shape
    dims, columns = tall.shape
    lanes = slice(half * columns, (half + 1) * columns)
    group = min(64, index_heads)
    tall[...] = jnp.zeros_like(tall)

    @pl.loop(0, index_heads // group)
    def _(step):
        gap = gap_ref[:, lanes]
        slopes = []
        for head in range(group):
            place = step * group + head
            scaled = gap * jnp.concatenate([scale_ref[place]] * (columns // LANES), axis=1)
            slope = jnp.where(active_ref[place, :, lanes] > 0.0, scaled, 0.0)
            slopes.append(slope if rows % 16 else slope.astype(jnp.bfloat16))
        slopes = jnp.concatenate(slopes, axis=0).astype(jnp.bfloat16)
        block = pl.ds(pl.multiple_of(step * (group * rows), group * rows), group * rows)
        slopes_ref[block, :] = slopes
        begin = pl.multiple_of(step * (group * dims), LANES)
        stacked = stack_heads(query_ref[:, pl.ds(begin, group * dims)], group, dims)
        tall[...] += lax.dot_general(
            stacked, slopes, (((0,), (0,)), ((), ())), preferred_element_type=jnp.float32
        )

    for place in range(columns // LANES):
        out_ref[lanes_of(place)] = jnp.transpose(tall[:, lanes_of(place)])


def key_terms(shares, gap, predicted, active, scales, index_query, dims, half):
    index_heads, rows, seq_total = active.shape
    columns = seq_total // 2
    out = (
        shape_of((index_heads * rows, columns), jnp.bfloat16),
        shape_of((columns, dims), jnp.float32),
    )
    if shares:
        out = (shape_of((rows, seq_total), jnp.float32), *out)
        args = (*shares, predicted)
    else:
        args = (gap,)
    return call(
        functools.partial(key_kernel, len(shares), half),
        out,
        (*args, active, scales, index_query),
        scratch=[pltpu.VMEM((dims, columns), jnp.float32)],
        flops=4 * rows * index_heads * seq_total * dims,
    )


def query_kernel(factor, gap_ref, even_ref, odd_ref, active_ref, keys_ref, grad_query_ref, grad_weight_ref, sums):
    index_heads, rows, seq_total = active_ref.shape
    dims = keys_ref.shape[1]
    group = min(64, index_heads)
    lane = lax.broadcasted_iota(jnp.int32, (rows, LANES), 1)
    sums[...] = jnp.zeros_like(sums)

    @pl.loop(0, index_heads // group)
    def _(step):
        gap = gap_ref[...]
        total = sums[...]
        for head in range(group):
            product = active_ref[step * group + head] * gap
            partial = functools.reduce(
                jnp.add, [product[:, lanes_of(place)] for place in range(seq_total // LANES)]
            )
            partial = jnp.sum(partial, axis=1, keepdims=True)
            total = jnp.where(lane == step * group + head, partial, total)
        sums[...] = total
        block = pl.ds(pl.multiple_of(step * (group * rows), group * rows), group * rows)
        slopes = jnp.concatenate([even_ref[block, :], odd_ref[block, :]], axis=1)
        grad = jnp.dot(slopes, keys_ref[...], preferred_element_type=jnp.float32)
        for head in range(group):
            begin = pl.multiple_of((step * group + head) * dims, dims)
            grad_query_ref[:, pl.ds(begin, dims)] = grad[head * rows : (head + 1) * rows]

    grad_weight_ref[...] = sums[:, :index_heads] * factor


def query_grads(gap, even, odd, active, keys, factor):
    index_heads, rows, seq_total = active.shape
    dims = keys.shape[1]
    return call(
        functools.partial(query_kernel, factor),
        (
            shape_of((rows, index_heads * dims), jnp.float32),
            shape_of((rows, index_heads), jnp.float32),
        ),
        (gap, even, odd, active, keys),
        scratch=[pltpu.VMEM((rows, LANES), jnp.float32)],
        flops=6 * rows * index_heads * seq_total * dims,
    )


def fold_kernel(keep_ref, come_ref, own_ref, *sends):
    total = keep_ref[...] + come_ref[...]
    rows = own_ref.shape[0]
    own_ref[...] = total[:rows]
    for hop, send in enumerate(sends):
        send[...] = total[(hop + 1) * rows : (hop + 2) * rows].astype(send.dtype)


def fold(keep, come, block):
    count = keep.shape[0] // block
    piece = (block, keep.shape[1])
    out = (shape_of(piece, jnp.float32),) + (shape_of(piece, jnp.bfloat16),) * (count - 1)
    return call(fold_kernel, out, (keep, come), flops=10_000_000)


def per_device(lat_query, lat_keys, normalizer, lookback, index_query, index_keys, index_weight):
    seq_count = lax.axis_size("seq")
    peers = lax.axis_size("head")
    heads = lat_query.shape[1] // KDIM
    rows, _ = index_weight.shape
    dims = index_keys.shape[1]
    factor = dims ** (-0.5)

    def swap(value, bits):
        return lax.ppermute(value, "seq", [(place, place ^ bits) for place in range(seq_count)])

    def pass_on(values):
        out = []
        for hop, value in enumerate(values):
            to = [(place, (place + hop + 1) % peers) for place in range(peers)]
            out.append(lax.ppermute(value, "head", to))
        return out

    mine = jnp.concatenate([lat_keys.T, index_keys], axis=0)
    blocks = {0: mine}
    for bits in range(2, seq_count, 2):
        blocks[bits] = swap(mine, bits)
    for bits in range(0, seq_count, 2):
        blocks[bits + 1] = swap(blocks[bits], 1)
    phases = [[0, 1], [2, 4], [3, 5], list(range(6, seq_count))]
    order = [*range(0, seq_count, 2), *range(1, seq_count, 2)]

    query, offsets, scales, lows = spread(
        lat_query, normalizer, index_weight, lookback, heads, factor
    )
    prior = []
    for phase in phases:
        last = phase is phases[-1]
        mass = attention_mass(
            query,
            offsets,
            [blocks[slot] for slot in phase],
            prior if last else [],
            [order.index(slot) for slots in phases for slot in slots] if last else [],
            rows,
            peers,
        )
        prior.append(mass)
    own, *sends = mass
    shares = [own, *pass_on(sends)]
    active, predicted, keys = index_scores(
        index_query, scales, lows, [blocks[slot] for slot in order], order, dims
    )
    terms = functools.partial(
        key_terms, active=active, scales=scales, index_query=index_query, dims=dims
    )
    gap, odd, give = terms(shares, None, predicted, half=1)
    come = swap(give, 1)
    even, keep = terms([], gap, None, half=0)
    own, *sends = fold(keep, come, LANES)
    others = [swap(send, 2 * (hop + 1)) for hop, send in enumerate(sends)]
    grad_query, grad_weight = query_grads(gap, even, odd, active, keys, factor)
    own, *sends = gather_terms(own, others, rows, peers)
    others = pass_on(sends)
    grad_key = functools.reduce(jnp.add, others, own)
    return grad_query, grad_weight, grad_key


def gather_kernel(peers, own_ref, *refs):
    others, (mine_ref, *sends), total = refs[: len(refs) - peers - 1], refs[-peers - 1 : -1], refs[-1]
    value = own_ref[...]
    for other in others:
        value = value + other[...].astype(jnp.float32)
    total[...] = value
    rows = mine_ref.shape[0]
    me = lax.axis_index("head")
    mine_ref[...] = total[pl.ds(me * rows, rows), :]
    for hop, send in enumerate(sends):
        send[...] = total[pl.ds(lax.rem(me + hop + 1, peers) * rows, rows), :]


def gather_terms(own, others, rows, peers):
    piece = shape_of((rows, own.shape[1]), jnp.float32)
    return call(
        functools.partial(gather_kernel, peers),
        (piece,) * peers,
        (own, *others),
        scratch=[pltpu.VMEM(own.shape, jnp.float32)],
        flops=10_000_000,
    )


def solution(mesh):
    return jax.shard_map(
        per_device,
        mesh=mesh,
        in_specs=(
            P("seq", "head"),
            P("seq", None),
            P("seq", None),
            P("seq"),
            P(("seq", "head"), None),
            P("seq", None),
            P(("seq", "head"), None),
        ),
        out_specs=(P(("seq", "head"), None), P(("seq", "head"), None), P(("seq", "head"), None)),
        check_vma=False,
    )
```

```python
import functools
import math

import jax
import jax.numpy as jnp
from jax import lax
from jax.experimental import pallas as pl
from jax.experimental.pallas import tpu as pltpu
from jax.sharding import PartitionSpec as P


KDIM = 576
LANES = 128
WIDE = 2 * LANES
PAD = LANES - KDIM % LANES
LOG2E = 1.0 / math.log(2.0)
HBM = pl.BlockSpec(memory_space=pltpu.HBM)
VMEM = pl.BlockSpec(memory_space=pltpu.VMEM)


def shape_of(dims, kind):
    return jax.ShapeDtypeStruct(dims, kind)


def call(body, out_shape, args, specs=None, out_specs=None, scratch=(), flops=0, limit=20):
    return pl.pallas_call(
        body,
        out_shape=out_shape,
        in_specs=specs or [VMEM] * len(args),
        out_specs=out_specs or jax.tree.map(lambda _: VMEM, out_shape),
        scratch_shapes=list(scratch),
        compiler_params=pltpu.CompilerParams(vmem_limit_bytes=limit << 20),
        cost_estimate=pl.CostEstimate(flops=flops, bytes_accessed=0, transcendentals=0),
    )(*args)


def lanes_of(place):
    return slice(place * LANES, (place + 1) * LANES)


def spread_kernel(factor, query_hbm, norm_hbm, weight_hbm, look_hbm, *refs):
    query_ref, off_ref, scale_ref, low_ref, norm, weight, look, tall, sems = refs
    pairs = ((norm_hbm, norm), (weight_hbm, weight), (look_hbm, look), (query_hbm, query_ref))
    copies = [pltpu.make_async_copy(*pair, sems.at[place]) for place, pair in enumerate(pairs)]
    for copy in copies:
        copy.start()
    heads, local_rows, _ = off_ref.shape
    rows = low_ref.shape[0]
    me = lax.axis_index("head")
    copies[0].wait()
    width = norm.shape[1]
    offsets = pltpu.roll(norm[...] * LOG2E, lax.rem(width - me * heads, width), 1)
    for head in range(heads):
        off_ref[head] = jnp.broadcast_to(offsets[:, head : head + 1], (local_rows, LANES))
    copies[1].wait()
    weights = weight[...] * factor
    for head in range(scale_ref.shape[0]):
        scale_ref[head] = jnp.broadcast_to(weights[:, head : head + 1], (rows, LANES))
    copies[2].wait()
    tall[...] = jnp.transpose(
        jnp.broadcast_to(look[...].astype(jnp.float32), (LANES, local_rows))
    )
    low_ref[...] = tall[pl.ds(me * rows, rows), :]
    copies[3].wait()


def spread(lat_query, normalizer, weight, lookback, heads, factor):
    rows, index_heads = weight.shape
    local_rows = normalizer.shape[0]
    look = lookback.reshape(1, local_rows)
    out = (
        shape_of(lat_query.shape, lat_query.dtype),
        shape_of((heads, local_rows, LANES), jnp.float32),
        shape_of((index_heads, rows, LANES), jnp.float32),
        shape_of((rows, LANES), jnp.float32),
    )
    scratch = [pltpu.VMEM(value.shape, value.dtype) for value in (normalizer, weight, look)]
    scratch += [pltpu.VMEM((local_rows, LANES), jnp.float32), pltpu.SemaphoreType.DMA((4,))]
    return call(
        functools.partial(spread_kernel, factor),
        out,
        tuple(pltpu.with_memory_space_constraint(value, pltpu.HBM) for value in (lat_query, normalizer, weight, look)),
        specs=[HBM] * 4,
        scratch=scratch,
        flops=1_500_000_000,
    )


def mass_kernel(slots, carried, places, query_ref, off_ref, *refs):
    blocks, refs = refs[:slots], refs[slots:]
    prior, refs = refs[:carried], refs[carried:]
    outs, (keys, acc) = refs[:-2], refs[-2:]
    tiles, local_rows, wide = acc.shape
    heads = off_ref.shape[0]
    group = min(32, heads)
    depth = KDIM + PAD
    per_tile = wide // LANES
    for tile in range(tiles):
        keys[tile, :PAD] = jnp.zeros((PAD, wide), keys.dtype)
        keys[tile, PAD + KDIM :] = jnp.zeros((PAD, wide), keys.dtype)
        for part in range(per_tile):
            keys[tile, PAD : PAD + KDIM, lanes_of(part)] = blocks[tile * per_tile + part][:KDIM]
    acc[...] = jnp.zeros_like(acc)
    scale = KDIM ** (-0.5) * LOG2E

    @pl.loop(0, heads // group)
    def _(step):
        @pl.loop(0, tiles)
        def _(tile):
            total = acc[tile]
            for odd in range(2):
                picked = []
                for head in range(odd, group, 2):
                    begin = step * (group * KDIM) + (head * KDIM - (PAD if odd else 0))
                    picked.append(query_ref[:, pl.ds(pl.multiple_of(begin, LANES), depth)])
                first = 0 if odd else PAD
                scores = jnp.dot(
                    jnp.concatenate(picked, axis=0),
                    keys[tile, first : first + depth],
                    preferred_element_type=jnp.float32,
                )
                for place, head in enumerate(range(odd, group, 2)):
                    offset = jnp.concatenate([off_ref[step * group + head]] * per_tile, axis=1)
                    part = scores[place * local_rows : (place + 1) * local_rows]
                    total = total + jnp.exp2(part * scale - offset)
            acc[tile] = total

    if not places:
        outs[0][...] = acc[...]
        return
    own, sends = outs[0], outs[1:]
    rows = own.shape[0]
    size = len(sends) + 1
    me = lax.axis_index("head")
    sources = [(ref, tile) for ref in (*prior, acc) for tile in range(ref.shape[0])]
    pieces = [(ref, tile, part) for ref, tile in sources for part in range(per_tile)]
    for place, (ref, tile, part) in zip(places, pieces):
        lanes = lanes_of(part)
        own[:, lanes_of(place)] = ref[tile, pl.ds(me * rows, rows), lanes]
        for hop, send in enumerate(sends):
            there = lax.rem(me + hop + 1, size)
            send[:, lanes_of(place)] = ref[tile, pl.ds(there * rows, rows), lanes].astype(send.dtype)


def attention_mass(query, offsets, blocks, prior, places, rows, peers):
    local_rows = query.shape[0]
    heads = offsets.shape[0]
    slots = len(blocks)
    tiles = slots * LANES // WIDE
    if places:
        columns = len(places) * LANES
        out = (shape_of((rows, columns), jnp.float32),)
        out += (shape_of((rows, columns), jnp.bfloat16),) * (peers - 1)
    else:
        out = shape_of((tiles, local_rows, WIDE), jnp.float32)
    return call(
        functools.partial(mass_kernel, slots, len(prior), places),
        out,
        (query, offsets, *blocks, *prior),
        scratch=[
            pltpu.VMEM((tiles, KDIM + 2 * PAD, WIDE), jnp.bfloat16),
            pltpu.VMEM((tiles, local_rows, WIDE), jnp.float32),
        ],
        flops=2 * local_rows * heads * KDIM * slots * LANES,
    )


def stack_heads(value, heads, dims):
    parts = [value[:, head * dims : (head + 1) * dims] for head in range(heads)]
    if value.shape[0] % 16 == 0:
        return jnp.concatenate(parts, axis=0)
    parts = [part.astype(jnp.float32) for part in parts]
    return jnp.concatenate(parts, axis=0).astype(value.dtype)


def score_kernel(slots, query_ref, scale_ref, *refs):
    blocks, (active_ref, score, keys) = refs[:slots], refs[slots:]
    score_blocks(blocks, query_ref, scale_ref, active_ref, score, keys)


def score_blocks(blocks, query_ref, scale_ref, active_ref, score, keys):
    index_heads, rows, columns = active_ref.shape
    dims = keys.shape[1]
    group = min(64, index_heads)
    score[...] = jnp.zeros_like(score)
    for place, block in enumerate(blocks):
        keys[lanes_of(place)] = block[KDIM:]

    @pl.loop(0, index_heads // group)
    def _(step):
        begin = pl.multiple_of(step * (group * dims), LANES)
        stacked = stack_heads(query_ref[:, pl.ds(begin, group * dims)], group, dims)
        for begin in range(0, columns, WIDE):
            inner = lax.dot_general(
                stacked,
                keys[begin : begin + WIDE],
                (((1,), (1,)), ((), ())),
                preferred_element_type=jnp.float32,
            )
            total = score[:, begin : begin + WIDE]
            for head in range(group):
                active = jnp.maximum(inner[head * rows : (head + 1) * rows], 0.0)
                active_ref[step * group + head, :, begin : begin + WIDE] = active
                total = total + active * jnp.concatenate([scale_ref[step * group + head]] * 2, axis=1)
            score[:, begin : begin + WIDE] = total


def predict_kernel(order, slots, query_ref, scale_ref, low_ref, first_ref, first_keys_ref, *refs):
    blocks, refs = refs[:slots], refs[slots:]
    active_ref, predicted_ref, keys_ref, score, keys = refs
    score_blocks(blocks, query_ref, scale_ref, active_ref, score, keys)
    rows = score.shape[0]
    halves = halved((first_ref, score), 1)
    for half in range(2):
        begin = half * (len(order) // 2) * LANES
        for ref in (first_keys_ref, keys):
            part = ref.shape[0] // 2
            keys_ref[begin : begin + part] = ref[half * part : (half + 1) * part]
            begin += part

    seq = lax.axis_index("seq")
    query_pos = (
        seq * lax.axis_size("head") + lax.axis_index("head")
    ) * rows + lax.broadcasted_iota(jnp.int32, (rows, LANES), 0)
    low = query_pos - low_ref[...].astype(jnp.int32)
    lane = lax.broadcasted_iota(jnp.int32, (rows, LANES), 1)
    scores = jnp.concatenate(halves, axis=1)
    parts, seen = [], []
    for place, slot in enumerate(order):
        key_pos = jnp.bitwise_xor(seq, slot) * LANES + lane
        seen.append((key_pos <= query_pos) & (key_pos >= low))
        parts.append(jnp.where(seen[-1], scores[:, lanes_of(place)], -jnp.inf))
    top = jnp.max(functools.reduce(jnp.maximum, parts), axis=1, keepdims=True)
    parts = [jnp.exp(part - top) for part in parts]
    mass = jnp.sum(functools.reduce(jnp.add, parts), axis=1, keepdims=True)
    for place in range(len(order)):
        predicted_ref[:, lanes_of(place)] = jnp.where(seen[place], parts[place] / mass, -1.0)


def halved(refs, axis, *index):
    out = []
    for half in range(2):
        parts = []
        for ref in refs:
            part = ref.shape[-1] // 2
            parts.append(ref[(*index, slice(None), slice(half * part, (half + 1) * part))])
        out.append(jnp.concatenate(parts, axis=axis))
    return out


def index_scores(index_query, scales, blocks, dims):
    rows = index_query.shape[0]
    index_heads = scales.shape[0]
    columns = len(blocks) * LANES
    return call(
        functools.partial(score_kernel, len(blocks)),
        (
            shape_of((index_heads, rows, columns), jnp.float32),
            shape_of((rows, columns), jnp.float32),
            shape_of((columns, dims), jnp.bfloat16),
        ),
        (index_query, scales, *blocks),
        flops=6 * rows * index_heads * columns * dims,
    )


def predictions(index_query, scales, lows, scores, keys, blocks, order, dims):
    rows = index_query.shape[0]
    index_heads = scales.shape[0]
    columns = len(blocks) * LANES
    seq_total = len(order) * LANES
    return call(
        functools.partial(predict_kernel, order, len(blocks)),
        (
            shape_of((index_heads, rows, columns), jnp.float32),
            shape_of((rows, seq_total), jnp.float32),
            shape_of((seq_total, dims), jnp.bfloat16),
        ),
        (index_query, scales, lows, scores, keys, *blocks),
        scratch=[
            pltpu.VMEM((rows, columns), jnp.float32),
            pltpu.VMEM((columns, dims), jnp.bfloat16),
        ],
        flops=8 * rows * index_heads * columns * dims,
    )


def gap_of(shares, peers, predicted):
    pieces = []
    for begin in range(0, len(shares), peers):
        mine, *others = shares[begin : begin + peers]
        mass = mine[...]
        for other in others:
            mass = mass + other[...].astype(jnp.float32)
        pieces.append(mass)
    seen = predicted >= 0.0
    mass = jnp.where(seen, jnp.concatenate(halved(pieces, 1), axis=1), 0.0)
    target = mass / jnp.sum(mass, axis=1, keepdims=True)
    return jnp.where(seen, predicted - target, 0.0)


def key_kernel(count, peers, half, *refs):
    shares, refs = refs[:count], refs[count:]
    if count:
        predicted_ref, *actives, scale_ref, query_ref, gap_ref, slopes_ref, out_ref, tall = refs
        gap_ref[...] = gap_of(shares, peers, predicted_ref[...])
    else:
        gap_ref, *actives, scale_ref, query_ref, slopes_ref, out_ref, tall = refs
    index_heads, rows, _ = actives[0].shape
    dims, columns = tall.shape
    lanes = slice(half * columns, (half + 1) * columns)
    group = min(64, index_heads)
    tall[...] = jnp.zeros_like(tall)

    @pl.loop(0, index_heads // group)
    def _(step):
        gap = gap_ref[:, lanes]
        slopes = []
        for head in range(group):
            place = step * group + head
            scaled = gap * jnp.concatenate([scale_ref[place]] * (columns // LANES), axis=1)
            slope = jnp.where(halved(actives, 1, place)[half] > 0.0, scaled, 0.0)
            slopes.append(slope if rows % 16 else slope.astype(jnp.bfloat16))
        slopes = jnp.concatenate(slopes, axis=0).astype(jnp.bfloat16)
        block = pl.ds(pl.multiple_of(step * (group * rows), group * rows), group * rows)
        slopes_ref[block, :] = slopes
        begin = pl.multiple_of(step * (group * dims), LANES)
        stacked = stack_heads(query_ref[:, pl.ds(begin, group * dims)], group, dims)
        tall[...] += lax.dot_general(
            stacked, slopes, (((0,), (0,)), ((), ())), preferred_element_type=jnp.float32
        )

    for place in range(columns // LANES):
        out_ref[lanes_of(place)] = jnp.transpose(tall[:, lanes_of(place)])


def key_terms(shares, gap, predicted, actives, scales, index_query, dims, peers, half):
    index_heads, rows, _ = actives[0].shape
    seq_total = sum(active.shape[2] for active in actives)
    columns = seq_total // 2
    out = (
        shape_of((index_heads * rows, columns), jnp.bfloat16),
        shape_of((columns, dims), jnp.float32),
    )
    if shares:
        out = (shape_of((rows, seq_total), jnp.float32), *out)
        args = (*shares, predicted)
    else:
        args = (gap,)
    return call(
        functools.partial(key_kernel, len(shares), peers, half),
        out,
        (*args, *actives, scales, index_query),
        scratch=[pltpu.VMEM((dims, columns), jnp.float32)],
        flops=4 * rows * index_heads * seq_total * dims,
    )


def query_kernel(pieces, even_ref, odd_ref, keys_ref, grad_query_hbm, grads, sems):
    rows, columns = grads.shape
    dims = keys_ref.shape[1]
    heads = columns // dims // pieces
    copies = []
    for piece in range(pieces):
        block = slice(piece * heads * rows, (piece + 1) * heads * rows)
        slopes = jnp.concatenate([even_ref[block], odd_ref[block]], axis=1)
        grad = jnp.dot(slopes, keys_ref[...], preferred_element_type=jnp.float32)
        for head in range(heads):
            begin = (piece * heads + head) * dims
            grads[:, begin : begin + dims] = grad[head * rows : (head + 1) * rows]
        lanes = pl.ds(piece * heads * dims, heads * dims)
        copy = pltpu.make_async_copy(grads.at[:, lanes], grad_query_hbm.at[:, lanes], sems.at[piece])
        copy.start()
        copies.append(copy)
    for copy in copies:
        copy.wait()


def query_grads(even, odd, keys, rows):
    columns = even.shape[0] // rows * keys.shape[1]
    pieces = 4
    return call(
        functools.partial(query_kernel, pieces),
        shape_of((rows, columns), jnp.float32),
        (even, odd, keys),
        out_specs=HBM,
        scratch=[pltpu.VMEM((rows, columns), jnp.float32), pltpu.SemaphoreType.DMA((pieces,))],
        flops=4 * even.shape[0] * keys.shape[0] * keys.shape[1],
    )


def weight_kernel(factor, gap_ref, *refs):
    *actives, grad_weight_ref, sums = refs
    index_heads, rows, _ = actives[0].shape
    group = min(64, index_heads)
    lane = lax.broadcasted_iota(jnp.int32, (rows, LANES), 1)
    sums[...] = jnp.zeros_like(sums)

    @pl.loop(0, index_heads // group)
    def _(step):
        gap = gap_ref[...]
        total = sums[...]
        for head in range(group):
            place = step * group + head
            product = jnp.concatenate(halved(actives, 1, place), axis=1) * gap
            partial = functools.reduce(
                jnp.add, [product[:, lanes_of(slot)] for slot in range(gap.shape[1] // LANES)]
            )
            partial = jnp.sum(partial, axis=1, keepdims=True)
            total = jnp.where(lane == place, partial, total)
        sums[...] = total

    grad_weight_ref[...] = sums[:, :index_heads] * factor


def weight_grads(gap, actives, factor):
    index_heads, rows, _ = actives[0].shape
    return call(
        functools.partial(weight_kernel, factor),
        shape_of((rows, index_heads), jnp.float32),
        (gap, *actives),
        scratch=[pltpu.VMEM((rows, LANES), jnp.float32)],
        flops=512 * rows * index_heads * gap.shape[1],
    )


def fold_kernel(keep_ref, come_ref, own_ref, *sends):
    total = keep_ref[...] + come_ref[...]
    rows = own_ref.shape[0]
    own_ref[...] = total[:rows]
    for hop, send in enumerate(sends):
        send[...] = total[(hop + 1) * rows : (hop + 2) * rows].astype(send.dtype)


def fold(keep, come, block):
    count = keep.shape[0] // block
    piece = (block, keep.shape[1])
    out = (shape_of(piece, jnp.float32),) + (shape_of(piece, jnp.bfloat16),) * (count - 1)
    return call(fold_kernel, out, (keep, come), flops=10_000_000)


def per_device(lat_query, lat_keys, normalizer, lookback, index_query, index_keys, index_weight):
    seq_count = lax.axis_size("seq")
    peers = lax.axis_size("head")
    heads = lat_query.shape[1] // KDIM
    rows, _ = index_weight.shape
    dims = index_keys.shape[1]
    factor = dims ** (-0.5)

    def swap(value, bits):
        return lax.ppermute(value, "seq", [(place, place ^ bits) for place in range(seq_count)])

    def pass_on(values):
        out = []
        for hop, value in enumerate(values):
            to = [(place, (place + hop + 1) % peers) for place in range(peers)]
            out.append(lax.ppermute(value, "head", to))
        return out

    mine = jnp.concatenate([lat_keys.T, index_keys], axis=0)
    blocks = {0: mine}
    for bits in range(2, seq_count, 2):
        blocks[bits] = swap(mine, bits)
    for bits in range(0, seq_count, 2):
        blocks[bits + 1] = swap(blocks[bits], 1)
    phases = [[0, 1], [2, 4], [3, 5], list(range(6, seq_count))]
    order = [*range(0, seq_count, 2), *range(1, seq_count, 2)]

    query, offsets, scales, lows = spread(
        lat_query, normalizer, index_weight, lookback, heads, factor
    )
    early = sorted((slot for phase in phases[:-1] for slot in phase), key=order.index)
    late = sorted(phases[-1], key=order.index)
    prior, shares = [], []
    for place, phase in enumerate(phases):
        ready = late if place == 3 else early if place == 2 else []
        since = [slot for slots in phases[:place] for slot in slots] if place == 2 else []
        mass = attention_mass(
            query,
            offsets,
            [blocks[slot] for slot in phase],
            prior if since else [],
            [ready.index(slot) for slot in since + phase] if ready else [],
            rows,
            peers,
        )
        if ready:
            shares += [mass[0], *pass_on(mass[1:])]
        else:
            prior.append(mass)
    first, scores, keys = index_scores(index_query, scales, [blocks[slot] for slot in early], dims)
    second, predicted, keys = predictions(
        index_query, scales, lows, scores, keys, [blocks[slot] for slot in late], order, dims
    )
    terms = functools.partial(
        key_terms, actives=(first, second), scales=scales, index_query=index_query, dims=dims, peers=peers
    )
    gap, odd, give = terms(shares, None, predicted, half=1)
    come = swap(give, 1)
    even, keep = terms([], gap, None, half=0)
    own, *sends = fold(keep, come, LANES)
    others = [swap(send, 2 * (hop + 1)) for hop, send in enumerate(sends)]
    grad_query = query_grads(even, odd, keys, rows)
    grad_weight = weight_grads(gap, (first, second), factor)
    own, *sends = gather_terms(own, others, rows, peers)
    others = pass_on(sends)
    grad_key = functools.reduce(jnp.add, others, own)
    return grad_query, grad_weight, grad_key


def gather_kernel(peers, own_ref, *refs):
    others, (mine_ref, *sends), total = refs[: len(refs) - peers - 1], refs[-peers - 1 : -1], refs[-1]
    value = own_ref[...]
    for other in others:
        value = value + other[...].astype(jnp.float32)
    total[...] = value
    rows = mine_ref.shape[0]
    me = lax.axis_index("head")
    mine_ref[...] = total[pl.ds(me * rows, rows), :]
    for hop, send in enumerate(sends):
        send[...] = total[pl.ds(lax.rem(me + hop + 1, peers) * rows, rows), :]


def gather_terms(own, others, rows, peers):
    piece = shape_of((rows, own.shape[1]), jnp.float32)
    return call(
        functools.partial(gather_kernel, peers),
        (piece,) * peers,
        (own, *others),
        scratch=[pltpu.VMEM(own.shape, jnp.float32)],
        flops=10_000_000,
    )


def solution(mesh):
    return jax.shard_map(
        per_device,
        mesh=mesh,
        in_specs=(
            P("seq", "head"),
            P("seq", None),
            P("seq", None),
            P("seq"),
            P(("seq", "head"), None),
            P("seq", None),
            P(("seq", "head"), None),
        ),
        out_specs=(P(("seq", "head"), None), P(("seq", "head"), None), P(("seq", "head"), None)),
        check_vma=False,
    )
```

```python
import functools
import math

import jax
import jax.numpy as jnp
from jax import lax
from jax.experimental import pallas as pl
from jax.experimental.pallas import tpu as pltpu
from jax.sharding import PartitionSpec as P


KDIM = 576
LANES = 128
WIDE = 2 * LANES
PAD = LANES - KDIM % LANES
LOG2E = 1.0 / math.log(2.0)
HBM = pl.BlockSpec(memory_space=pltpu.HBM)
VMEM = pl.BlockSpec(memory_space=pltpu.VMEM)


def shape_of(dims, kind):
    return jax.ShapeDtypeStruct(dims, kind)


def call(body, out_shape, args, specs=None, scratch=(), flops=0, limit=20):
    return pl.pallas_call(
        body,
        out_shape=out_shape,
        in_specs=specs or [VMEM] * len(args),
        out_specs=jax.tree.map(lambda _: VMEM, out_shape),
        scratch_shapes=list(scratch),
        compiler_params=pltpu.CompilerParams(vmem_limit_bytes=limit << 20),
        cost_estimate=pl.CostEstimate(flops=flops, bytes_accessed=0, transcendentals=0),
    )(*args)


def lanes_of(place):
    return slice(place * LANES, (place + 1) * LANES)


def spread_kernel(factor, query_hbm, norm_hbm, weight_hbm, look_hbm, *refs):
    query_ref, off_ref, scale_ref, low_ref, norm, weight, look, tall, sems = refs
    pairs = ((norm_hbm, norm), (weight_hbm, weight), (look_hbm, look), (query_hbm, query_ref))
    copies = [pltpu.make_async_copy(*pair, sems.at[place]) for place, pair in enumerate(pairs)]
    for copy in copies:
        copy.start()
    heads, local_rows, _ = off_ref.shape
    rows = low_ref.shape[0]
    me = lax.axis_index("head")
    copies[0].wait()
    width = norm.shape[1]
    offsets = pltpu.roll(norm[...] * LOG2E, lax.rem(width - me * heads, width), 1)
    for head in range(heads):
        off_ref[head] = jnp.broadcast_to(offsets[:, head : head + 1], (local_rows, LANES))
    copies[1].wait()
    weights = weight[...] * factor
    for head in range(scale_ref.shape[0]):
        scale_ref[head] = jnp.broadcast_to(weights[:, head : head + 1], (rows, LANES))
    copies[2].wait()
    tall[...] = jnp.transpose(
        jnp.broadcast_to(look[...].astype(jnp.float32), (LANES, local_rows))
    )
    low_ref[...] = tall[pl.ds(me * rows, rows), :]
    copies[3].wait()


def spread(lat_query, normalizer, weight, lookback, heads, factor):
    rows, index_heads = weight.shape
    local_rows = normalizer.shape[0]
    look = lookback.reshape(1, local_rows)
    out = (
        shape_of(lat_query.shape, lat_query.dtype),
        shape_of((heads, local_rows, LANES), jnp.float32),
        shape_of((index_heads, rows, LANES), jnp.float32),
        shape_of((rows, LANES), jnp.float32),
    )
    scratch = [pltpu.VMEM(value.shape, value.dtype) for value in (normalizer, weight, look)]
    scratch += [pltpu.VMEM((local_rows, LANES), jnp.float32), pltpu.SemaphoreType.DMA((4,))]
    return call(
        functools.partial(spread_kernel, factor),
        out,
        tuple(pltpu.with_memory_space_constraint(value, pltpu.HBM) for value in (lat_query, normalizer, weight, look)),
        specs=[HBM] * 4,
        scratch=scratch,
        flops=1_500_000_000,
    )


def mass_kernel(slots, carried, places, query_ref, off_ref, *refs):
    blocks, refs = refs[:slots], refs[slots:]
    prior, refs = refs[:carried], refs[carried:]
    outs, (keys, acc) = refs[:-2], refs[-2:]
    tiles, local_rows, wide = acc.shape
    heads = off_ref.shape[0]
    group = min(32, heads)
    depth = KDIM + PAD
    per_tile = wide // LANES
    for tile in range(tiles):
        keys[tile, :PAD] = jnp.zeros((PAD, wide), keys.dtype)
        keys[tile, PAD + KDIM :] = jnp.zeros((PAD, wide), keys.dtype)
        for part in range(per_tile):
            keys[tile, PAD : PAD + KDIM, lanes_of(part)] = blocks[tile * per_tile + part][:KDIM]
    acc[...] = jnp.zeros_like(acc)
    scale = KDIM ** (-0.5) * LOG2E

    @pl.loop(0, heads // group)
    def _(step):
        @pl.loop(0, tiles)
        def _(tile):
            total = acc[tile]
            for odd in range(2):
                picked = []
                for head in range(odd, group, 2):
                    begin = step * (group * KDIM) + (head * KDIM - (PAD if odd else 0))
                    picked.append(query_ref[:, pl.ds(pl.multiple_of(begin, LANES), depth)])
                first = 0 if odd else PAD
                scores = jnp.dot(
                    jnp.concatenate(picked, axis=0),
                    keys[tile, first : first + depth],
                    preferred_element_type=jnp.float32,
                )
                for place, head in enumerate(range(odd, group, 2)):
                    offset = jnp.concatenate([off_ref[step * group + head]] * per_tile, axis=1)
                    part = scores[place * local_rows : (place + 1) * local_rows]
                    total = total + jnp.exp2(part * scale - offset)
            acc[tile] = total

    if not places:
        outs[0][...] = acc[...]
        return
    own, sends = outs[0], outs[1:]
    rows = own.shape[0]
    size = len(sends) + 1
    me = lax.axis_index("head")
    sources = [(ref, tile) for ref in (*prior, acc) for tile in range(ref.shape[0])]
    pieces = [(ref, tile, part) for ref, tile in sources for part in range(per_tile)]
    for place, (ref, tile, part) in zip(places, pieces):
        lanes = lanes_of(part)
        own[:, lanes_of(place)] = ref[tile, pl.ds(me * rows, rows), lanes]
        for hop, send in enumerate(sends):
            there = lax.rem(me + hop + 1, size)
            send[:, lanes_of(place)] = ref[tile, pl.ds(there * rows, rows), lanes].astype(send.dtype)


def attention_mass(query, offsets, blocks, prior, places, rows, peers):
    local_rows = query.shape[0]
    heads = offsets.shape[0]
    slots = len(blocks)
    tiles = slots * LANES // WIDE
    if places:
        columns = len(places) * LANES
        out = (shape_of((rows, columns), jnp.float32),)
        out += (shape_of((rows, columns), jnp.bfloat16),) * (peers - 1)
    else:
        out = shape_of((tiles, local_rows, WIDE), jnp.float32)
    return call(
        functools.partial(mass_kernel, slots, len(prior), places),
        out,
        (query, offsets, *blocks, *prior),
        scratch=[
            pltpu.VMEM((tiles, KDIM + 2 * PAD, WIDE), jnp.bfloat16),
            pltpu.VMEM((tiles, local_rows, WIDE), jnp.float32),
        ],
        flops=2 * local_rows * heads * KDIM * slots * LANES,
    )


def stack_heads(value, heads, dims):
    parts = [value[:, head * dims : (head + 1) * dims] for head in range(heads)]
    if value.shape[0] % 16 == 0:
        return jnp.concatenate(parts, axis=0)
    parts = [part.astype(jnp.float32) for part in parts]
    return jnp.concatenate(parts, axis=0).astype(value.dtype)


def score_kernel(order, query_ref, scale_ref, low_ref, *refs):
    slots = len(order)
    blocks = refs[:slots]
    active_ref, predicted_ref, keys, score = refs[slots:]
    index_heads, rows, seq_total = active_ref.shape
    dims = keys.shape[1]
    group = min(64, index_heads)
    score[...] = jnp.zeros_like(score)
    for place in range(slots):
        keys[lanes_of(place)] = blocks[place][KDIM:]

    @pl.loop(0, index_heads // group)
    def _(step):
        begin = pl.multiple_of(step * (group * dims), LANES)
        stacked = stack_heads(query_ref[:, pl.ds(begin, group * dims)], group, dims)
        for begin in range(0, seq_total, WIDE):
            inner = lax.dot_general(
                stacked,
                keys[begin : begin + WIDE],
                (((1,), (1,)), ((), ())),
                preferred_element_type=jnp.float32,
            )
            total = score[:, begin : begin + WIDE]
            for head in range(group):
                active = jnp.maximum(inner[head * rows : (head + 1) * rows], 0.0)
                active_ref[step * group + head, :, begin : begin + WIDE] = active
                total = total + active * jnp.concatenate([scale_ref[step * group + head]] * 2, axis=1)
            score[:, begin : begin + WIDE] = total

    seq = lax.axis_index("seq")
    query_pos = (
        seq * lax.axis_size("head") + lax.axis_index("head")
    ) * rows + lax.broadcasted_iota(jnp.int32, (rows, LANES), 0)
    low = query_pos - low_ref[...].astype(jnp.int32)
    lane = lax.broadcasted_iota(jnp.int32, (rows, LANES), 1)
    seen = []
    for slot in order:
        key_pos = jnp.bitwise_xor(seq, slot) * LANES + lane
        seen.append((key_pos <= query_pos) & (key_pos >= low))
    parts = [score[:, lanes_of(place)] for place in range(slots)]
    parts = [jnp.where(see, part, -jnp.inf) for see, part in zip(seen, parts)]
    top = jnp.max(functools.reduce(jnp.maximum, parts), axis=1, keepdims=True)
    parts = [jnp.exp(part - top) for part in parts]
    mass = jnp.sum(functools.reduce(jnp.add, parts), axis=1, keepdims=True)
    for place in range(slots):
        predicted_ref[:, lanes_of(place)] = jnp.where(seen[place], parts[place] / mass, -1.0)


def index_scores(index_query, scales, lows, blocks, order, dims):
    rows = index_query.shape[0]
    index_heads = scales.shape[0]
    seq_total = len(order) * LANES
    return call(
        functools.partial(score_kernel, order),
        (
            shape_of((index_heads, rows, seq_total), jnp.float32),
            shape_of((rows, seq_total), jnp.float32),
            shape_of((seq_total, dims), jnp.bfloat16),
        ),
        (index_query, scales, lows, *blocks),
        scratch=[pltpu.VMEM((rows, seq_total), jnp.float32)],
        flops=6 * rows * index_heads * seq_total * dims,
    )


def gap_of(shares, predicted):
    mine, *others = shares
    mass = mine[...]
    for other in others:
        mass = mass + other[...].astype(jnp.float32)
    seen = predicted >= 0.0
    mass = jnp.where(seen, mass, 0.0)
    target = mass / jnp.sum(mass, axis=1, keepdims=True)
    return jnp.where(seen, predicted - target, 0.0)


def key_kernel(peers, half, *refs):
    shares, refs = refs[:peers], refs[peers:]
    if peers:
        predicted_ref, active_ref, scale_ref, query_ref, gap_ref, slopes_ref, out_ref, tall = refs
        gap_ref[...] = gap_of(shares, predicted_ref[...])
    else:
        gap_ref, active_ref, scale_ref, query_ref, slopes_ref, out_ref, tall = refs
    index_heads, rows, _ = active_ref.shape
    dims, columns = tall.shape
    lanes = slice(half * columns, (half + 1) * columns)
    group = min(64, index_heads)
    tall[...] = jnp.zeros_like(tall)

    @pl.loop(0, index_heads // group)
    def _(step):
        gap = gap_ref[:, lanes]
        slopes = []
        for head in range(group):
            place = step * group + head
            scaled = gap * jnp.concatenate([scale_ref[place]] * (columns // LANES), axis=1)
            slope = jnp.where(active_ref[place, :, lanes] > 0.0, scaled, 0.0)
            slopes.append(slope if rows % 16 else slope.astype(jnp.bfloat16))
        slopes = jnp.concatenate(slopes, axis=0).astype(jnp.bfloat16)
        block = pl.ds(pl.multiple_of(step * (group * rows), group * rows), group * rows)
        slopes_ref[block, :] = slopes
        begin = pl.multiple_of(step * (group * dims), LANES)
        stacked = stack_heads(query_ref[:, pl.ds(begin, group * dims)], group, dims)
        tall[...] += lax.dot_general(
            stacked, slopes, (((0,), (0,)), ((), ())), preferred_element_type=jnp.float32
        )

    for place in range(columns // LANES):
        out_ref[lanes_of(place)] = jnp.transpose(tall[:, lanes_of(place)])


def key_terms(shares, gap, predicted, active, scales, index_query, dims, half):
    index_heads, rows, seq_total = active.shape
    columns = seq_total // 2
    out = (
        shape_of((index_heads * rows, columns), jnp.bfloat16),
        shape_of((columns, dims), jnp.float32),
    )
    if shares:
        out = (shape_of((rows, seq_total), jnp.float32), *out)
        args = (*shares, predicted)
    else:
        args = (gap,)
    return call(
        functools.partial(key_kernel, len(shares), half),
        out,
        (*args, active, scales, index_query),
        scratch=[pltpu.VMEM((dims, columns), jnp.float32)],
        flops=4 * rows * index_heads * seq_total * dims,
    )


def query_kernel(factor, gap_ref, even_ref, odd_ref, active_ref, keys_ref, grad_query_ref, grad_weight_ref, sums):
    index_heads, rows, seq_total = active_ref.shape
    dims = keys_ref.shape[1]
    group = min(64, index_heads)
    lane = lax.broadcasted_iota(jnp.int32, (rows, LANES), 1)
    sums[...] = jnp.zeros_like(sums)

    @pl.loop(0, index_heads // group)
    def _(step):
        gap = gap_ref[...]
        total = sums[...]
        for head in range(group):
            product = active_ref[step * group + head] * gap
            partial = functools.reduce(
                jnp.add, [product[:, lanes_of(place)] for place in range(seq_total // LANES)]
            )
            partial = jnp.sum(partial, axis=1, keepdims=True)
            total = jnp.where(lane == step * group + head, partial, total)
        sums[...] = total
        block = pl.ds(pl.multiple_of(step * (group * rows), group * rows), group * rows)
        slopes = jnp.concatenate([even_ref[block, :], odd_ref[block, :]], axis=1)
        grad = jnp.dot(slopes, keys_ref[...], preferred_element_type=jnp.float32)
        for head in range(group):
            begin = pl.multiple_of((step * group + head) * dims, dims)
            grad_query_ref[:, pl.ds(begin, dims)] = grad[head * rows : (head + 1) * rows]

    grad_weight_ref[...] = sums[:, :index_heads] * factor


def query_grads(gap, even, odd, active, keys, factor):
    index_heads, rows, seq_total = active.shape
    dims = keys.shape[1]
    return call(
        functools.partial(query_kernel, factor),
        (
            shape_of((rows, index_heads * dims), jnp.float32),
            shape_of((rows, index_heads), jnp.float32),
        ),
        (gap, even, odd, active, keys),
        scratch=[pltpu.VMEM((rows, LANES), jnp.float32)],
        flops=6 * rows * index_heads * seq_total * dims,
    )


def fold_kernel(keep_ref, come_ref, out_ref):
    place = lax.axis_index("seq") // 2
    for chip in range(out_ref.shape[0] // LANES):
        begin = pl.multiple_of(jnp.bitwise_xor(place, chip) * LANES, LANES)
        total = keep_ref[lanes_of(chip)] + come_ref[lanes_of(chip)]
        out_ref[pl.ds(begin, LANES), :] = total.astype(out_ref.dtype)


def fold(keep, come):
    out = shape_of(keep.shape, jnp.bfloat16)
    return call(fold_kernel, out, (keep, come), flops=10_000_000)


def per_device(lat_query, lat_keys, normalizer, lookback, index_query, index_keys, index_weight):
    seq_count = lax.axis_size("seq")
    peers = lax.axis_size("head")
    heads = lat_query.shape[1] // KDIM
    rows, _ = index_weight.shape
    dims = index_keys.shape[1]
    factor = dims ** (-0.5)

    def swap(value, bits):
        return lax.ppermute(value, "seq", [(place, place ^ bits) for place in range(seq_count)])

    def pass_on(values):
        out = []
        for hop, value in enumerate(values):
            to = [(place, (place + hop + 1) % peers) for place in range(peers)]
            out.append(lax.ppermute(value, "head", to))
        return out

    mine = jnp.concatenate([lat_keys.T, index_keys], axis=0)
    blocks = {0: mine}
    for bits in range(2, seq_count, 2):
        blocks[bits] = swap(mine, bits)
    for bits in range(0, seq_count, 2):
        blocks[bits + 1] = swap(blocks[bits], 1)
    phases = [[0, 1], [2, 3], [*range(4, seq_count, 2)], [*range(5, seq_count, 2)]]
    order = [*range(0, seq_count, 2), *range(1, seq_count, 2)]

    query, offsets, scales, lows = spread(
        lat_query, normalizer, index_weight, lookback, heads, factor
    )
    prior = []
    for phase in phases:
        last = phase is phases[-1]
        mass = attention_mass(
            query,
            offsets,
            [blocks[slot] for slot in phase],
            prior if last else [],
            [order.index(slot) for slots in phases for slot in slots] if last else [],
            rows,
            peers,
        )
        prior.append(mass)
    own, *sends = mass
    shares = [own, *pass_on(sends)]
    active, predicted, keys = index_scores(
        index_query, scales, lows, [blocks[slot] for slot in order], order, dims
    )
    terms = functools.partial(
        key_terms, active=active, scales=scales, index_query=index_query, dims=dims
    )
    gap, odd, give = terms(shares, None, predicted, half=1)
    come = swap(give, 1)
    even, keep = terms([], gap, None, half=0)
    members = [
        [seq * peers + head for seq in range(core, seq_count, 2) for head in range(peers)]
        for core in range(2)
    ]
    arrived = lax.all_to_all(
        fold(keep, come), ("seq", "head"), 0, 0, tiled=True, axis_index_groups=members
    )
    grad_query, grad_weight = query_grads(gap, even, odd, active, keys, factor)
    grad_key = jnp.sum(arrived.reshape(-1, rows, dims).astype(jnp.float32), axis=0)
    return grad_query, grad_weight, grad_key


def solution(mesh):
    return jax.shard_map(
        per_device,
        mesh=mesh,
        in_specs=(
            P("seq", "head"),
            P("seq", None),
            P("seq", None),
            P("seq"),
            P(("seq", "head"), None),
            P("seq", None),
            P(("seq", "head"), None),
        ),
        out_specs=(P(("seq", "head"), None), P(("seq", "head"), None), P(("seq", "head"), None)),
        check_vma=False,
    )
```

```python
import functools
import math

import jax
import jax.numpy as jnp
from jax import lax
from jax.experimental import pallas as pl
from jax.experimental.pallas import tpu as pltpu
from jax.sharding import PartitionSpec as P


KDIM = 576
LANES = 128
WIDE = 2 * LANES
PAD = LANES - KDIM % LANES
LOG2E = 1.0 / math.log(2.0)
QUERY_COPIES = 8
HBM = pl.BlockSpec(memory_space=pltpu.HBM)
VMEM = pl.BlockSpec(memory_space=pltpu.VMEM)


def shape_of(dims, kind):
    return jax.ShapeDtypeStruct(dims, kind)


def call(body, out_shape, args, specs=None, out_specs=None, scratch=(), flops=0, limit=20):
    return pl.pallas_call(
        body,
        out_shape=out_shape,
        in_specs=specs or [VMEM] * len(args),
        out_specs=out_specs or jax.tree.map(lambda _: VMEM, out_shape),
        scratch_shapes=list(scratch),
        compiler_params=pltpu.CompilerParams(vmem_limit_bytes=limit << 20),
        cost_estimate=pl.CostEstimate(flops=flops, bytes_accessed=0, transcendentals=0),
    )(*args)


def lanes_of(place):
    return slice(place * LANES, (place + 1) * LANES)


def spread_kernel(factor, query_hbm, norm_hbm, weight_hbm, look_hbm, *refs):
    query_ref, off_ref, scale_ref, low_ref, norm, weight, look, tall, sems = refs
    pairs = [(norm_hbm, norm), (weight_hbm, weight), (look_hbm, look)]
    chunk = query_ref.shape[0] // QUERY_COPIES
    for part in range(QUERY_COPIES):
        block = pl.ds(part * chunk, chunk)
        pairs.append((query_hbm.at[block], query_ref.at[block]))
    copies = [pltpu.make_async_copy(*pair, sems.at[place]) for place, pair in enumerate(pairs)]
    for copy in copies:
        copy.start()
    heads, local_rows, _ = off_ref.shape
    rows = low_ref.shape[0]
    me = lax.axis_index("head")
    copies[0].wait()
    width = norm.shape[1]
    offsets = pltpu.roll(norm[...] * LOG2E, lax.rem(width - me * heads, width), 1)
    for head in range(heads):
        off_ref[head] = jnp.broadcast_to(offsets[:, head : head + 1], (local_rows, LANES))
    copies[1].wait()
    weights = weight[...] * factor
    for head in range(scale_ref.shape[0]):
        scale_ref[head] = jnp.broadcast_to(weights[:, head : head + 1], (rows, LANES))
    copies[2].wait()
    tall[...] = jnp.transpose(
        jnp.broadcast_to(look[...].astype(jnp.float32), (LANES, local_rows))
    )
    low_ref[...] = tall[pl.ds(me * rows, rows), :]
    for copy in copies[3:]:
        copy.wait()


def spread(lat_query, normalizer, weight, lookback, heads, factor):
    rows, index_heads = weight.shape
    local_rows = normalizer.shape[0]
    look = lookback.reshape(1, local_rows)
    out = (
        shape_of(lat_query.shape, lat_query.dtype),
        shape_of((heads, local_rows, LANES), jnp.float32),
        shape_of((index_heads, rows, LANES), jnp.float32),
        shape_of((rows, LANES), jnp.float32),
    )
    scratch = [pltpu.VMEM(value.shape, value.dtype) for value in (normalizer, weight, look)]
    scratch += [pltpu.VMEM((local_rows, LANES), jnp.float32), pltpu.SemaphoreType.DMA((3 + QUERY_COPIES,))]
    return call(
        functools.partial(spread_kernel, factor),
        out,
        tuple(pltpu.with_memory_space_constraint(value, pltpu.HBM) for value in (lat_query, normalizer, weight, look)),
        specs=[HBM] * 4,
        scratch=scratch,
        flops=1_500_000_000,
    )


def mass_kernel(slots, carried, places, query_ref, off_ref, *refs):
    blocks, refs = refs[:slots], refs[slots:]
    prior, refs = refs[:carried], refs[carried:]
    outs, (keys, acc) = refs[:-2], refs[-2:]
    tiles, local_rows, wide = acc.shape
    heads = off_ref.shape[0]
    group = min(32, heads)
    depth = KDIM + PAD
    per_tile = wide // LANES
    for tile in range(tiles):
        keys[tile, :PAD] = jnp.zeros((PAD, wide), keys.dtype)
        keys[tile, PAD + KDIM :] = jnp.zeros((PAD, wide), keys.dtype)
        for part in range(per_tile):
            keys[tile, PAD : PAD + KDIM, lanes_of(part)] = blocks[tile * per_tile + part][:KDIM]
    acc[...] = jnp.zeros_like(acc)
    scale = KDIM ** (-0.5) * LOG2E

    @pl.loop(0, heads // group)
    def _(step):
        @pl.loop(0, tiles)
        def _(tile):
            total = acc[tile]
            for odd in range(2):
                picked = []
                for head in range(odd, group, 2):
                    begin = step * (group * KDIM) + (head * KDIM - (PAD if odd else 0))
                    picked.append(query_ref[:, pl.ds(pl.multiple_of(begin, LANES), depth)])
                first = 0 if odd else PAD
                scores = jnp.dot(
                    jnp.concatenate(picked, axis=0),
                    keys[tile, first : first + depth],
                    preferred_element_type=jnp.float32,
                )
                for place, head in enumerate(range(odd, group, 2)):
                    offset = jnp.concatenate([off_ref[step * group + head]] * per_tile, axis=1)
                    part = scores[place * local_rows : (place + 1) * local_rows]
                    total = total + jnp.exp2(part * scale - offset)
            acc[tile] = total

    if not places:
        outs[0][...] = acc[...]
        return
    own, sends = outs[0], outs[1:]
    rows = own.shape[0]
    me = lax.axis_index("head")
    sources = [(ref, tile) for ref in (*prior, acc) for tile in range(ref.shape[0])]
    pieces = [(ref, tile, part) for ref, tile in sources for part in range(per_tile)]
    for place, (ref, tile, part) in zip(places, pieces):
        lanes = lanes_of(part)
        own[:, lanes_of(place)] = ref[tile, pl.ds(me * rows, rows), lanes]
        for hop, send in enumerate(sends):
            there = lax.rem(me + hop + 1, lax.axis_size("head"))
            send[:, lanes_of(place)] = ref[tile, pl.ds(there * rows, rows), lanes].astype(send.dtype)


def attention_mass(query, offsets, blocks, prior, places, rows, peers):
    local_rows = query.shape[0]
    heads = offsets.shape[0]
    slots = len(blocks)
    tiles = slots * LANES // WIDE
    if places:
        columns = len(places) * LANES
        out = (shape_of((rows, columns), jnp.float32),)
        out += (shape_of((rows, columns), jnp.bfloat16),) * (peers - 1)
    else:
        out = shape_of((tiles, local_rows, WIDE), jnp.float32)
    return call(
        functools.partial(mass_kernel, slots, len(prior), places),
        out,
        (query, offsets, *blocks, *prior),
        scratch=[
            pltpu.VMEM((tiles, KDIM + 2 * PAD, WIDE), jnp.bfloat16),
            pltpu.VMEM((tiles, local_rows, WIDE), jnp.float32),
        ],
        flops=2 * local_rows * heads * KDIM * slots * LANES,
    )


def stack_heads(value, heads, dims):
    parts = [value[:, head * dims : (head + 1) * dims] for head in range(heads)]
    if value.shape[0] % 16 == 0:
        return jnp.concatenate(parts, axis=0)
    parts = [part.astype(jnp.float32) for part in parts]
    return jnp.concatenate(parts, axis=0).astype(value.dtype)


def score_kernel(order, query_ref, scale_ref, low_ref, *refs):
    slots = len(order)
    blocks = refs[:slots]
    active_ref, predicted_ref, keys, score = refs[slots:]
    index_heads, rows, seq_total = active_ref.shape
    dims = keys.shape[1]
    group = min(64, index_heads)
    score[...] = jnp.zeros_like(score)
    for place in range(slots):
        keys[lanes_of(place)] = blocks[place][KDIM:]

    @pl.loop(0, index_heads // group)
    def _(step):
        begin = pl.multiple_of(step * (group * dims), LANES)
        stacked = stack_heads(query_ref[:, pl.ds(begin, group * dims)], group, dims)
        for begin in range(0, seq_total, WIDE):
            inner = lax.dot_general(
                stacked,
                keys[begin : begin + WIDE],
                (((1,), (1,)), ((), ())),
                preferred_element_type=jnp.float32,
            )
            total = score[:, begin : begin + WIDE]
            for head in range(group):
                active = jnp.maximum(inner[head * rows : (head + 1) * rows], 0.0)
                active_ref[step * group + head, :, begin : begin + WIDE] = active
                total = total + active * jnp.concatenate([scale_ref[step * group + head]] * 2, axis=1)
            score[:, begin : begin + WIDE] = total

    seq = lax.axis_index("seq")
    query_pos = (
        seq * lax.axis_size("head") + lax.axis_index("head")
    ) * rows + lax.broadcasted_iota(jnp.int32, (rows, LANES), 0)
    low = query_pos - low_ref[...].astype(jnp.int32)
    lane = lax.broadcasted_iota(jnp.int32, (rows, LANES), 1)
    seen = []
    for slot in order:
        key_pos = jnp.bitwise_xor(seq, slot) * LANES + lane
        seen.append((key_pos <= query_pos) & (key_pos >= low))
    parts = [score[:, lanes_of(place)] for place in range(slots)]
    parts = [jnp.where(see, part, -jnp.inf) for see, part in zip(seen, parts)]
    top = jnp.max(functools.reduce(jnp.maximum, parts), axis=1, keepdims=True)
    parts = [jnp.exp(part - top) for part in parts]
    mass = jnp.sum(functools.reduce(jnp.add, parts), axis=1, keepdims=True)
    for place in range(slots):
        predicted_ref[:, lanes_of(place)] = jnp.where(seen[place], parts[place] / mass, -1.0)


def index_scores(index_query, scales, lows, blocks, order, dims):
    rows = index_query.shape[0]
    index_heads = scales.shape[0]
    seq_total = len(order) * LANES
    return call(
        functools.partial(score_kernel, order),
        (
            shape_of((index_heads, rows, seq_total), jnp.float32),
            shape_of((rows, seq_total), jnp.float32),
            shape_of((seq_total, dims), jnp.bfloat16),
        ),
        (index_query, scales, lows, *blocks),
        scratch=[pltpu.VMEM((rows, seq_total), jnp.float32)],
        flops=6 * rows * index_heads * seq_total * dims,
    )


def gap_of(shares, predicted):
    mine, *others = shares
    mass = mine[...]
    for other in others:
        mass = mass + other[...].astype(jnp.float32)
    seen = predicted >= 0.0
    mass = jnp.where(seen, mass, 0.0)
    target = mass / jnp.sum(mass, axis=1, keepdims=True)
    return jnp.where(seen, predicted - target, 0.0)


def key_kernel(peers, half, *refs):
    shares, refs = refs[:peers], refs[peers:]
    if peers:
        predicted_ref, active_ref, scale_ref, query_ref, gap_ref, out_ref, tall = refs
        gap_ref[...] = gap_of(shares, predicted_ref[...])
    else:
        gap_ref, active_ref, scale_ref, query_ref, out_ref, tall = refs
    index_heads, rows, _ = active_ref.shape
    dims, columns = tall.shape
    lanes = slice(half * columns, (half + 1) * columns)
    group = min(64, index_heads)
    tall[...] = jnp.zeros_like(tall)

    @pl.loop(0, index_heads // group)
    def _(step):
        gap = gap_ref[:, lanes]
        slopes = []
        for head in range(group):
            place = step * group + head
            scaled = gap * jnp.concatenate([scale_ref[place]] * (columns // LANES), axis=1)
            slope = jnp.where(active_ref[place, :, lanes] > 0.0, scaled, 0.0)
            slopes.append(slope if rows % 16 else slope.astype(jnp.bfloat16))
        slopes = jnp.concatenate(slopes, axis=0).astype(jnp.bfloat16)
        begin = pl.multiple_of(step * (group * dims), LANES)
        stacked = stack_heads(query_ref[:, pl.ds(begin, group * dims)], group, dims)
        tall[...] += lax.dot_general(
            stacked, slopes, (((0,), (0,)), ((), ())), preferred_element_type=jnp.float32
        )

    for place in range(columns // LANES):
        out_ref[lanes_of(place)] = jnp.transpose(tall[:, lanes_of(place)])


def key_terms(shares, gap, predicted, active, scales, index_query, dims, half):
    index_heads, rows, seq_total = active.shape
    columns = seq_total // 2
    out = (shape_of((columns, dims), jnp.float32),)
    if shares:
        out = (shape_of((rows, seq_total), jnp.float32), *out)
        args = (*shares, predicted)
    else:
        args = (gap,)
    return call(
        functools.partial(key_kernel, len(shares), half),
        out,
        (*args, active, scales, index_query),
        scratch=[pltpu.VMEM((dims, columns), jnp.float32)],
        flops=4 * rows * index_heads * seq_total * dims,
    )


def query_kernel(pieces, factor, query_hbm, keys_hbm, gap_hbm, weight_hbm, *refs):
    grad_query_hbm, grad_weight_ref, query, keys, gap, weight, slopes, grads, scales, sems = refs
    pairs = ((query_hbm, query), (keys_hbm, keys), (weight_hbm, weight), (gap_hbm, gap))
    copies = [pltpu.make_async_copy(*pair, sems.at[place]) for place, pair in enumerate(pairs)]
    for copy in copies:
        copy.start()
    for copy in copies:
        copy.wait()
    rows, index_heads = weight.shape
    seq_total, dims = keys.shape
    heads = index_heads // pieces
    lane = lax.broadcasted_iota(jnp.int32, (rows, LANES), 1)
    sums = jnp.zeros((rows, LANES), jnp.float32)
    weights = weight[...] * factor
    for head in range(index_heads):
        scales[head] = jnp.broadcast_to(weights[:, head : head + 1], (rows, LANES))
    copies = []
    for piece in range(pieces):
        lanes = slice(piece * heads * dims, (piece + 1) * heads * dims)
        stacked = stack_heads(query[:, lanes], heads, dims)
        partial = [jnp.zeros((rows, LANES), jnp.float32)] * heads
        for begin in range(0, seq_total, WIDE):
            inner = lax.dot_general(
                stacked,
                keys[begin : begin + WIDE],
                (((1,), (1,)), ((), ())),
                preferred_element_type=jnp.float32,
            )
            part = gap[:, begin : begin + WIDE]
            for head in range(heads):
                place = piece * heads + head
                active = jnp.maximum(inner[head * rows : (head + 1) * rows], 0.0)
                product = active * part
                partial[head] = partial[head] + (product[:, :LANES] + product[:, LANES:])
                scaled = part * jnp.concatenate([scales[place]] * 2, axis=1)
                slope = jnp.where(active > 0.0, scaled, 0.0)
                slopes[head * rows : (head + 1) * rows, begin : begin + WIDE] = slope.astype(slopes.dtype)
        grad = jnp.dot(slopes[...].astype(keys.dtype), keys[...], preferred_element_type=jnp.float32)
        for head in range(heads):
            begin = (piece * heads + head) * dims
            grads[:, begin : begin + dims] = grad[head * rows : (head + 1) * rows]
            total = jnp.sum(partial[head], axis=1, keepdims=True)
            sums = jnp.where(lane == piece * heads + head, total, sums)
        lanes = pl.ds(piece * heads * dims, heads * dims)
        copy = pltpu.make_async_copy(grads.at[:, lanes], grad_query_hbm.at[:, lanes], sems.at[4 + piece])
        copy.start()
        copies.append(copy)
    grad_weight_ref[...] = sums[:, :index_heads] * factor
    for copy in copies:
        copy.wait()


def query_grads(index_query, keys, gap, weight, factor):
    rows, index_heads = weight.shape
    seq_total, dims = keys.shape
    pieces = 2
    args = (index_query, keys, gap, weight)
    kind = jnp.float32 if rows % 16 else jnp.bfloat16
    scratch = [pltpu.VMEM(value.shape, value.dtype) for value in args]
    scratch += [
        pltpu.VMEM((index_heads // pieces * rows, seq_total), kind),
        pltpu.VMEM((rows, index_heads * dims), jnp.float32),
        pltpu.VMEM((index_heads, rows, LANES), jnp.float32),
        pltpu.SemaphoreType.DMA((4 + pieces,)),
    ]
    return call(
        functools.partial(query_kernel, pieces, factor),
        (
            shape_of((rows, index_heads * dims), jnp.float32),
            shape_of((rows, index_heads), jnp.float32),
        ),
        tuple(pltpu.with_memory_space_constraint(value, pltpu.HBM) for value in args),
        specs=[HBM] * 4,
        out_specs=(HBM, VMEM),
        scratch=scratch,
        flops=8 * rows * index_heads * seq_total * dims,
    )


def fold_kernel(keep_ref, come_ref, out_ref):
    place = lax.axis_index("seq") // 2
    for chip in range(out_ref.shape[0] // LANES):
        begin = pl.multiple_of(jnp.bitwise_xor(place, chip) * LANES, LANES)
        total = keep_ref[lanes_of(chip)] + come_ref[lanes_of(chip)]
        out_ref[pl.ds(begin, LANES), :] = total.astype(out_ref.dtype)


def fold(keep, come):
    out = shape_of(keep.shape, jnp.bfloat16)
    return call(fold_kernel, out, (keep, come), flops=10_000_000)


def per_device(lat_query, lat_keys, normalizer, lookback, index_query, index_keys, index_weight):
    seq_count = lax.axis_size("seq")
    peers = lax.axis_size("head")
    heads = lat_query.shape[1] // KDIM
    rows, _ = index_weight.shape
    dims = index_keys.shape[1]
    factor = dims ** (-0.5)

    def swap(value, bits):
        return lax.ppermute(value, "seq", [(place, place ^ bits) for place in range(seq_count)])

    def pass_on(values, pair):
        out = []
        for hop, value in enumerate(values):
            to = [(place, pair(place, hop + 1)) for place in range(peers)]
            out.append(lax.ppermute(value, "head", to))
        return out

    mine = jnp.concatenate([lat_keys.T, index_keys], axis=0)
    blocks = {0: mine}
    for bits in range(2, seq_count, 2):
        blocks[bits] = swap(mine, bits)
    for bits in range(0, seq_count, 2):
        blocks[bits + 1] = swap(blocks[bits], 1)
    phases = [[0, 1], [2, 4], [3, 5], [*range(6, seq_count)]]
    order = [*range(0, seq_count, 2), *range(1, seq_count, 2)]

    query, offsets, scales, lows = spread(
        lat_query, normalizer, index_weight, lookback, heads, factor
    )
    prior = []
    for phase in phases:
        last = phase is phases[-1]
        mass = attention_mass(
            query,
            offsets,
            [blocks[slot] for slot in phase],
            prior if last else [],
            [order.index(slot) for slots in phases for slot in slots] if last else [],
            rows,
            peers,
        )
        prior.append(mass)
    own, *sends = mass
    shares = [own, *pass_on(sends, lambda place, hop: (place + hop) % peers)]
    active, predicted, keys = index_scores(
        index_query, scales, lows, [blocks[slot] for slot in order], order, dims
    )
    terms = functools.partial(
        key_terms, active=active, scales=scales, index_query=index_query, dims=dims
    )
    gap, give = terms(shares, None, predicted, half=1)
    come = swap(give, 1)
    (keep,) = terms([], gap, None, half=0)
    members = [
        [seq * peers + head for seq in range(core, seq_count, 2) for head in range(peers)]
        for core in range(2)
    ]
    arrived = lax.all_to_all(
        fold(keep, come), ("seq", "head"), 0, 0, tiled=True, axis_index_groups=members
    )
    grad_query, grad_weight = query_grads(index_query, keys, gap, index_weight, factor)
    grad_key = jnp.sum(arrived.reshape(-1, rows, dims).astype(jnp.float32), axis=0)
    return grad_query, grad_weight, grad_key


def solution(mesh):
    return jax.shard_map(
        per_device,
        mesh=mesh,
        in_specs=(
            P("seq", "head"),
            P("seq", None),
            P("seq", None),
            P("seq"),
            P(("seq", "head"), None),
            P("seq", None),
            P(("seq", "head"), None),
        ),
        out_specs=(P(("seq", "head"), None), P(("seq", "head"), None), P(("seq", "head"), None)),
        check_vma=False,
    )
```

```python
import functools
import math

import jax
import jax.numpy as jnp
from jax import lax
from jax.experimental import pallas as pl
from jax.experimental.pallas import tpu as pltpu
from jax.sharding import PartitionSpec as P


KDIM = 576
LANES = 128
WIDE = 2 * LANES
PAD = LANES - KDIM % LANES
LOG2E = 1.0 / math.log(2.0)
QUERY_COPIES = 8
HBM = pl.BlockSpec(memory_space=pltpu.HBM)
VMEM = pl.BlockSpec(memory_space=pltpu.VMEM)


def shape_of(dims, kind):
    return jax.ShapeDtypeStruct(dims, kind)


def call(body, out_shape, args, specs=None, out_specs=None, scratch=(), flops=0, limit=20):
    return pl.pallas_call(
        body,
        out_shape=out_shape,
        in_specs=specs or [VMEM] * len(args),
        out_specs=out_specs or jax.tree.map(lambda _: VMEM, out_shape),
        scratch_shapes=list(scratch),
        compiler_params=pltpu.CompilerParams(vmem_limit_bytes=limit << 20),
        cost_estimate=pl.CostEstimate(flops=flops, bytes_accessed=0, transcendentals=0),
    )(*args)


def lanes_of(place):
    return slice(place * LANES, (place + 1) * LANES)


def spread_kernel(factor, query_hbm, norm_hbm, weight_hbm, look_hbm, *refs):
    query_ref, off_ref, scale_ref, low_ref, norm, weight, look, tall, sems = refs
    pairs = [(norm_hbm, norm), (weight_hbm, weight), (look_hbm, look)]
    chunk = query_ref.shape[0] // QUERY_COPIES
    for part in range(QUERY_COPIES):
        block = pl.ds(part * chunk, chunk)
        pairs.append((query_hbm.at[block], query_ref.at[block]))
    copies = [pltpu.make_async_copy(*pair, sems.at[place]) for place, pair in enumerate(pairs)]
    for copy in copies:
        copy.start()
    heads, local_rows, _ = off_ref.shape
    rows = low_ref.shape[0]
    me = lax.axis_index("head")
    copies[0].wait()
    width = norm.shape[1]
    offsets = pltpu.roll(norm[...] * LOG2E, lax.rem(width - me * heads, width), 1)
    for head in range(heads):
        off_ref[head] = jnp.broadcast_to(offsets[:, head : head + 1], (local_rows, LANES))
    copies[1].wait()
    weights = weight[...] * factor
    for head in range(scale_ref.shape[0]):
        scale_ref[head] = jnp.broadcast_to(weights[:, head : head + 1], (rows, LANES))
    copies[2].wait()
    tall[...] = jnp.transpose(
        jnp.broadcast_to(look[...].astype(jnp.float32), (LANES, local_rows))
    )
    low_ref[...] = tall[pl.ds(me * rows, rows), :]
    for copy in copies[3:]:
        copy.wait()


def spread(lat_query, normalizer, weight, lookback, heads, factor):
    rows, index_heads = weight.shape
    local_rows = normalizer.shape[0]
    look = lookback.reshape(1, local_rows)
    out = (
        shape_of(lat_query.shape, lat_query.dtype),
        shape_of((heads, local_rows, LANES), jnp.float32),
        shape_of((index_heads, rows, LANES), jnp.float32),
        shape_of((rows, LANES), jnp.float32),
    )
    scratch = [pltpu.VMEM(value.shape, value.dtype) for value in (normalizer, weight, look)]
    scratch += [pltpu.VMEM((local_rows, LANES), jnp.float32), pltpu.SemaphoreType.DMA((3 + QUERY_COPIES,))]
    return call(
        functools.partial(spread_kernel, factor),
        out,
        tuple(pltpu.with_memory_space_constraint(value, pltpu.HBM) for value in (lat_query, normalizer, weight, look)),
        specs=[HBM] * 4,
        scratch=scratch,
        flops=1_500_000_000,
    )


def mass_kernel(slots, carried, places, query_ref, off_ref, *refs):
    blocks, refs = refs[:slots], refs[slots:]
    prior, refs = refs[:carried], refs[carried:]
    outs, (keys, acc) = refs[:-2], refs[-2:]
    tiles, local_rows, wide = acc.shape
    heads = off_ref.shape[0]
    group = min(8, heads)
    depth = KDIM + PAD
    per_tile = wide // LANES
    for tile in range(tiles):
        keys[tile, :PAD] = jnp.zeros((PAD, wide), keys.dtype)
        keys[tile, PAD + KDIM :] = jnp.zeros((PAD, wide), keys.dtype)
        for part in range(per_tile):
            keys[tile, PAD : PAD + KDIM, lanes_of(part)] = blocks[tile * per_tile + part][:KDIM]
    scale = KDIM ** (-0.5) * LOG2E

    for tile in range(tiles):
        total = jnp.zeros((local_rows, wide), jnp.float32)
        for step in range(heads // group):
            for odd in range(2):
                mine = [step * group + head for head in range(odd, group, 2)]
                starts = [head * KDIM - (PAD if odd else 0) for head in mine]
                first = 0 if odd else PAD
                scores = jnp.dot(
                    jnp.concatenate([query_ref[:, at : at + depth] for at in starts], axis=0),
                    keys[tile, first : first + depth],
                    preferred_element_type=jnp.float32,
                )
                for place, head in enumerate(mine):
                    offset = jnp.concatenate([off_ref[head]] * per_tile, axis=1)
                    part = scores[place * local_rows : (place + 1) * local_rows]
                    total = total + jnp.exp2(part * scale - offset)
        acc[tile] = total

    if not places:
        outs[0][...] = acc[...]
        return
    own, sends = outs[0], outs[1:]
    rows = own.shape[0]
    me = lax.axis_index("head")
    sources = [(ref, tile) for ref in (*prior, acc) for tile in range(ref.shape[0])]
    pieces = [(ref, tile, part) for ref, tile in sources for part in range(per_tile)]
    for place, (ref, tile, part) in zip(places, pieces):
        lanes = lanes_of(part)
        own[:, lanes_of(place)] = ref[tile, pl.ds(me * rows, rows), lanes]
        for hop, send in enumerate(sends):
            there = lax.rem(me + hop + 1, lax.axis_size("head"))
            send[:, lanes_of(place)] = ref[tile, pl.ds(there * rows, rows), lanes].astype(send.dtype)


def attention_mass(query, offsets, blocks, prior, places, rows, peers):
    local_rows = query.shape[0]
    heads = offsets.shape[0]
    slots = len(blocks)
    tiles = slots * LANES // WIDE
    if places:
        columns = len(places) * LANES
        out = (shape_of((rows, columns), jnp.float32),)
        out += (shape_of((rows, columns), jnp.bfloat16),) * (peers - 1)
    else:
        out = shape_of((tiles, local_rows, WIDE), jnp.float32)
    return call(
        functools.partial(mass_kernel, slots, len(prior), places),
        out,
        (query, offsets, *blocks, *prior),
        scratch=[
            pltpu.VMEM((tiles, KDIM + 2 * PAD, WIDE), jnp.bfloat16),
            pltpu.VMEM((tiles, local_rows, WIDE), jnp.float32),
        ],
        flops=2 * local_rows * heads * KDIM * slots * LANES,
    )


def stack_heads(value, heads, dims):
    parts = [value[:, head * dims : (head + 1) * dims] for head in range(heads)]
    if value.shape[0] % 16 == 0:
        return jnp.concatenate(parts, axis=0)
    parts = [part.astype(jnp.float32) for part in parts]
    return jnp.concatenate(parts, axis=0).astype(value.dtype)


def score_kernel(order, query_ref, scale_ref, low_ref, *refs):
    slots = len(order)
    blocks = refs[:slots]
    active_ref, predicted_ref, keys, score = refs[slots:]
    index_heads, rows, seq_total = active_ref.shape
    dims = keys.shape[1]
    group = min(64, index_heads)
    score[...] = jnp.zeros_like(score)
    for place in range(slots):
        keys[lanes_of(place)] = blocks[place][KDIM:]

    @pl.loop(0, index_heads // group)
    def _(step):
        begin = pl.multiple_of(step * (group * dims), LANES)
        stacked = stack_heads(query_ref[:, pl.ds(begin, group * dims)], group, dims)
        for begin in range(0, seq_total, WIDE):
            inner = lax.dot_general(
                stacked,
                keys[begin : begin + WIDE],
                (((1,), (1,)), ((), ())),
                preferred_element_type=jnp.float32,
            )
            total = score[:, begin : begin + WIDE]
            for head in range(group):
                active = jnp.maximum(inner[head * rows : (head + 1) * rows], 0.0)
                active_ref[step * group + head, :, begin : begin + WIDE] = active
                total = total + active * jnp.concatenate([scale_ref[step * group + head]] * 2, axis=1)
            score[:, begin : begin + WIDE] = total

    seq = lax.axis_index("seq")
    query_pos = (
        seq * lax.axis_size("head") + lax.axis_index("head")
    ) * rows + lax.broadcasted_iota(jnp.int32, (rows, LANES), 0)
    low = query_pos - low_ref[...].astype(jnp.int32)
    lane = lax.broadcasted_iota(jnp.int32, (rows, LANES), 1)
    seen = []
    for slot in order:
        key_pos = jnp.bitwise_xor(seq, slot) * LANES + lane
        seen.append((key_pos <= query_pos) & (key_pos >= low))
    parts = [score[:, lanes_of(place)] for place in range(slots)]
    parts = [jnp.where(see, part, -jnp.inf) for see, part in zip(seen, parts)]
    top = jnp.max(functools.reduce(jnp.maximum, parts), axis=1, keepdims=True)
    parts = [jnp.exp(part - top) for part in parts]
    mass = jnp.sum(functools.reduce(jnp.add, parts), axis=1, keepdims=True)
    for place in range(slots):
        predicted_ref[:, lanes_of(place)] = jnp.where(seen[place], parts[place] / mass, -1.0)


def index_scores(index_query, scales, lows, blocks, order, dims):
    rows = index_query.shape[0]
    index_heads = scales.shape[0]
    seq_total = len(order) * LANES
    return call(
        functools.partial(score_kernel, order),
        (
            shape_of((index_heads, rows, seq_total), jnp.float32),
            shape_of((rows, seq_total), jnp.float32),
            shape_of((seq_total, dims), jnp.bfloat16),
        ),
        (index_query, scales, lows, *blocks),
        scratch=[pltpu.VMEM((rows, seq_total), jnp.float32)],
        flops=6 * rows * index_heads * seq_total * dims,
    )


def gap_of(shares, predicted):
    mine, *others = shares
    mass = mine[...]
    for other in others:
        mass = mass + other[...].astype(jnp.float32)
    seen = predicted >= 0.0
    mass = jnp.where(seen, mass, 0.0)
    target = mass / jnp.sum(mass, axis=1, keepdims=True)
    return jnp.where(seen, predicted - target, 0.0)


def key_kernel(peers, half, *refs):
    shares, refs = refs[:peers], refs[peers:]
    if peers:
        predicted_ref, active_ref, scale_ref, query_ref, gap_ref, out_ref, tall = refs
        gap_ref[...] = gap_of(shares, predicted_ref[...])
    else:
        gap_ref, active_ref, scale_ref, query_ref, out_ref, tall = refs
    index_heads, rows, _ = active_ref.shape
    dims, columns = tall.shape
    lanes = slice(half * columns, (half + 1) * columns)
    group = min(64, index_heads)
    tall[...] = jnp.zeros_like(tall)

    @pl.loop(0, index_heads // group)
    def _(step):
        gap = gap_ref[:, lanes]
        slopes = []
        for head in range(group):
            place = step * group + head
            scaled = gap * jnp.concatenate([scale_ref[place]] * (columns // LANES), axis=1)
            slope = jnp.where(active_ref[place, :, lanes] > 0.0, scaled, 0.0)
            slopes.append(slope if rows % 16 else slope.astype(jnp.bfloat16))
        slopes = jnp.concatenate(slopes, axis=0).astype(jnp.bfloat16)
        begin = pl.multiple_of(step * (group * dims), LANES)
        stacked = stack_heads(query_ref[:, pl.ds(begin, group * dims)], group, dims)
        tall[...] += lax.dot_general(
            stacked, slopes, (((0,), (0,)), ((), ())), preferred_element_type=jnp.float32
        )

    for place in range(columns // LANES):
        out_ref[lanes_of(place)] = jnp.transpose(tall[:, lanes_of(place)]).astype(out_ref.dtype)


def key_terms(shares, gap, predicted, active, scales, index_query, dims, half):
    index_heads, rows, seq_total = active.shape
    columns = seq_total // 2
    out = (shape_of((columns, dims), jnp.bfloat16 if half else jnp.float32),)
    if shares:
        out = (shape_of((rows, seq_total), jnp.float32), *out)
        args = (*shares, predicted)
    else:
        args = (gap,)
    return call(
        functools.partial(key_kernel, len(shares), half),
        out,
        (*args, active, scales, index_query),
        scratch=[pltpu.VMEM((dims, columns), jnp.float32)],
        flops=4 * rows * index_heads * seq_total * dims,
    )


def query_kernel(pieces, factor, query_hbm, keys_hbm, gap_hbm, weight_hbm, *refs):
    grad_query_hbm, grad_weight_ref, query, keys, gap, weight, slopes, grads, scales, sems = refs
    pairs = ((query_hbm, query), (keys_hbm, keys), (weight_hbm, weight), (gap_hbm, gap))
    copies = [pltpu.make_async_copy(*pair, sems.at[place]) for place, pair in enumerate(pairs)]
    for copy in copies:
        copy.start()
    for copy in copies:
        copy.wait()
    rows, index_heads = weight.shape
    seq_total, dims = keys.shape
    heads = index_heads // pieces
    lane = lax.broadcasted_iota(jnp.int32, (rows, LANES), 1)
    sums = jnp.zeros((rows, LANES), jnp.float32)
    weights = weight[...] * factor
    for head in range(index_heads):
        scales[head] = jnp.broadcast_to(weights[:, head : head + 1], (rows, LANES))
    copies = []
    for piece in range(pieces):
        lanes = slice(piece * heads * dims, (piece + 1) * heads * dims)
        stacked = stack_heads(query[:, lanes], heads, dims)
        partial = [jnp.zeros((rows, LANES), jnp.float32)] * heads
        for begin in range(0, seq_total, WIDE):
            inner = lax.dot_general(
                stacked,
                keys[begin : begin + WIDE],
                (((1,), (1,)), ((), ())),
                preferred_element_type=jnp.float32,
            )
            part = gap[:, begin : begin + WIDE]
            for head in range(heads):
                place = piece * heads + head
                active = jnp.maximum(inner[head * rows : (head + 1) * rows], 0.0)
                product = active * part
                partial[head] = partial[head] + (product[:, :LANES] + product[:, LANES:])
                scaled = part * jnp.concatenate([scales[place]] * 2, axis=1)
                slope = jnp.where(active > 0.0, scaled, 0.0)
                slopes[head * rows : (head + 1) * rows, begin : begin + WIDE] = slope.astype(slopes.dtype)
        grad = jnp.dot(slopes[...].astype(keys.dtype), keys[...], preferred_element_type=jnp.float32)
        for head in range(heads):
            begin = (piece * heads + head) * dims
            grads[:, begin : begin + dims] = grad[head * rows : (head + 1) * rows]
            total = jnp.sum(partial[head], axis=1, keepdims=True)
            sums = jnp.where(lane == piece * heads + head, total, sums)
        lanes = pl.ds(piece * heads * dims, heads * dims)
        copy = pltpu.make_async_copy(grads.at[:, lanes], grad_query_hbm.at[:, lanes], sems.at[4 + piece])
        copy.start()
        copies.append(copy)
    grad_weight_ref[...] = sums[:, :index_heads] * factor
    for copy in copies:
        copy.wait()


def query_grads(index_query, keys, gap, weight, factor):
    rows, index_heads = weight.shape
    seq_total, dims = keys.shape
    pieces = 2
    args = (index_query, keys, gap, weight)
    kind = jnp.float32 if rows % 16 else jnp.bfloat16
    scratch = [pltpu.VMEM(value.shape, value.dtype) for value in args]
    scratch += [
        pltpu.VMEM((index_heads // pieces * rows, seq_total), kind),
        pltpu.VMEM((rows, index_heads * dims), jnp.float32),
        pltpu.VMEM((index_heads, rows, LANES), jnp.float32),
        pltpu.SemaphoreType.DMA((4 + pieces,)),
    ]
    return call(
        functools.partial(query_kernel, pieces, factor),
        (
            shape_of((rows, index_heads * dims), jnp.float32),
            shape_of((rows, index_heads), jnp.float32),
        ),
        tuple(pltpu.with_memory_space_constraint(value, pltpu.HBM) for value in args),
        specs=[HBM] * 4,
        out_specs=(HBM, VMEM),
        scratch=scratch,
        flops=8 * rows * index_heads * seq_total * dims,
    )


def fold_kernel(keep_ref, come_ref, out_ref):
    place = lax.axis_index("seq") // 2
    for chip in range(out_ref.shape[0] // LANES):
        begin = pl.multiple_of(jnp.bitwise_xor(place, chip) * LANES, LANES)
        total = keep_ref[lanes_of(chip)] + come_ref[lanes_of(chip)].astype(jnp.float32)
        out_ref[pl.ds(begin, LANES), :] = total.astype(out_ref.dtype)


def fold(keep, come):
    out = shape_of(keep.shape, jnp.bfloat16)
    return call(fold_kernel, out, (keep, come), flops=10_000_000)


def per_device(lat_query, lat_keys, normalizer, lookback, index_query, index_keys, index_weight):
    seq_count = lax.axis_size("seq")
    peers = lax.axis_size("head")
    heads = lat_query.shape[1] // KDIM
    rows, _ = index_weight.shape
    dims = index_keys.shape[1]
    factor = dims ** (-0.5)

    def swap(value, bits):
        return lax.ppermute(value, "seq", [(place, place ^ bits) for place in range(seq_count)])

    def pass_on(values, pair):
        out = []
        for hop, value in enumerate(values):
            to = [(place, pair(place, hop + 1)) for place in range(peers)]
            out.append(lax.ppermute(value, "head", to))
        return out

    mine = jnp.concatenate([lat_keys.T, index_keys], axis=0)
    blocks = {0: mine}
    for bits in range(2, seq_count, 2):
        blocks[bits] = swap(mine, bits)
    for bits in range(0, seq_count, 2):
        blocks[bits + 1] = swap(blocks[bits], 1)
    phases = [[0, 1], [2, 4], [3, 5], [*range(6, seq_count)]]
    order = [*range(0, seq_count, 2), *range(1, seq_count, 2)]

    query, offsets, scales, lows = spread(
        lat_query, normalizer, index_weight, lookback, heads, factor
    )
    prior = []
    for phase in phases:
        last = phase is phases[-1]
        mass = attention_mass(
            query,
            offsets,
            [blocks[slot] for slot in phase],
            prior if last else [],
            [order.index(slot) for slots in phases for slot in slots] if last else [],
            rows,
            peers,
        )
        prior.append(mass)
    own, *sends = mass
    shares = [own, *pass_on(sends, lambda place, hop: (place + hop) % peers)]
    active, predicted, keys = index_scores(
        index_query, scales, lows, [blocks[slot] for slot in order], order, dims
    )
    terms = functools.partial(
        key_terms, active=active, scales=scales, index_query=index_query, dims=dims
    )
    gap, give = terms(shares, None, predicted, half=1)
    come = swap(give, 1)
    (keep,) = terms([], gap, None, half=0)
    members = [
        [seq * peers + head for seq in range(core, seq_count, 2) for head in range(peers)]
        for core in range(2)
    ]
    arrived = lax.all_to_all(
        fold(keep, come), ("seq", "head"), 0, 0, tiled=True, axis_index_groups=members
    )
    grad_query, grad_weight = query_grads(index_query, keys, gap, index_weight, factor)
    grad_key = jnp.sum(arrived.reshape(-1, rows, dims).astype(jnp.float32), axis=0)
    return grad_query, grad_weight, grad_key


def solution(mesh):
    return jax.shard_map(
        per_device,
        mesh=mesh,
        in_specs=(
            P("seq", "head"),
            P("seq", None),
            P("seq", None),
            P("seq"),
            P(("seq", "head"), None),
            P("seq", None),
            P(("seq", "head"), None),
        ),
        out_specs=(P(("seq", "head"), None), P(("seq", "head"), None), P(("seq", "head"), None)),
        check_vma=False,
    )
```
